512 devices in a mesh: dp: 4 (over y_lo, core), lat: 16 (over z), chan: 8 (over y_hi, x).
Axes of the slice: x: 4, y: 4 (y_hi: 2, y_lo: 2; y = y_hi * 2 + y_lo), z: 16, core: 2. Of those that a mesh axis runs over, the one named last changes fastest.
Arguments:
- saved_input: bfloat16 [4, 64, 720, 1024], P('dp', None, 'lat', 'chan'), may hold values from -6 to 6
- grad_output: bfloat16 [4, 64, 720, 1024], P('dp', None, 'lat', 'chan'), may hold values from -6 to 6
- legendre: bfloat16 [64, 192, 720], P('lat'), may hold values from -0.21875 to 0.21875
- quad_weight: float32 [720], replicated, may hold values from 0.3 to 3
- mixing_weight: bfloat16 [192, 512, 1024], P('lat', None, 'chan'), may hold values from -0.375 to 0.375
Outputs:
- grad_weight: bfloat16 [192, 512, 1024], P('lat', 'dp', 'chan')
- grad_input: bfloat16 [4, 64, 720, 1024], P('dp', None, 'lat', 'chan')
The draws below stay inside these ranges and needn't reach their ends.
All inputs are finite; a program needn't handle non-finite values.
Results may differ from the reference program's by a relative error of at most 0.014.
Values may be sent and summed in bfloat16 or wider, within the bound.
A program may use at most 64 MiB of HBM per device.

```python
import math
import jax
import jax.numpy as jnp
from jax import lax

NLAT = 720
L = 192
C = 512
BATCH = 4
M = 64
N_DP = 4
N_CHAN = 8


def strengthened(result, rng, source, target, blocks, factor):
    def block_of(axis_at):
        return (jnp.arange(result.shape[axis_at]) // (result.shape[axis_at] // blocks)).reshape((-1,) + (1,) * (result.ndim - 1 - axis_at))

    first = jax.random.permutation(rng, blocks)[block_of(target)]
    other_side = (block_of(target) + blocks // 2) % blocks
    return jnp.where((block_of(source) == first) | (block_of(source) == other_side), factor * result, result)


def level_of(rng, extent, split, low, top_value):
    def one(axis_at, blocks):
        draws = jax.random.uniform(jax.random.fold_in(jax.random.fold_in(rng, 6), axis_at), (blocks,), jnp.float32, low / len(split), top_value / len(split))
        return jnp.repeat(jnp.exp(draws), extent[axis_at] // blocks).reshape((-1,) + (1,) * (len(extent) - axis_at - 1))

    gain = one(*split[0])
    for cut in split[1:]:
        gain = gain * one(*cut)
    return gain


def gaussian(key, shape, scale, limit, shards=(), held_as=jnp.bfloat16):
    factor_of = level_of(key, shape, shards, -0.22, 0.18) if shards else 1.0
    values = jax.random.normal(key, shape, jnp.float32) * scale * factor_of
    return jnp.minimum(jnp.maximum(values, -limit), limit).astype(held_as)


def bell_draw_with(stream_key, extent, deviation, limit, split, heavy, dtype=jnp.bfloat16):
    values = deviation * jax.random.normal(stream_key, extent, jnp.float32)
    if split:
        values = values * level_of(stream_key, extent, split, -0.22, 0.18)
    return jnp.clip(strengthened(values, jax.random.fold_in(stream_key, 3), *heavy), -limit, limit).astype(dtype)


def setup_inputs(seed: int = 0) -> dict:
    key_list = jax.random.split(jax.random.key(seed), 6)
    saved_input = bell_draw_with(key_list[0], (BATCH, M, NLAT, 2 * C), 1.0, 6.0, ((0, 4), (2, 16), (3, 8)), (0, 3, 4, 2.0))
    grad_output = gaussian(key_list[1], (BATCH, M, NLAT, 2 * C), 1.0, 6.0, ((0, 4), (2, 16), (3, 8)))
    legendre = gaussian(key_list[2], (M, L, NLAT), NLAT ** -0.5, 0.21875, ((0, 16),))
    quad_weight = jnp.clip(jnp.exp(jax.random.uniform(key_list[3], (NLAT,), jnp.float32, math.log(0.3), math.log(3.0))), 0.3, 3.0)
    mixing_weight = bell_draw_with(key_list[4], (L, C, 2 * C), C ** -0.5, 0.375, ((0, 16), (2, 8)), (2, 1, 8, 2.0))
    return {"saved_input": saved_input, "grad_output": grad_output, "legendre": legendre, "quad_weight": quad_weight, "mixing_weight": mixing_weight}


def partner_of(grads):
    pairs = grads.reshape(grads.shape[:-1] + (grads.shape[-1] // 2, 2))
    swapped = jnp.stack([pairs[..., 1], -pairs[..., 0]], axis=-1)
    return swapped.reshape(grads.shape)


def weight_terms(spectra, grads):
    pairs = spectra.reshape(spectra.shape[:-1] + (spectra.shape[-1] // 2, 2))
    partner = partner_of(grads)
    first = jnp.einsum('bmli,bmlq->liq', pairs[..., 0], grads)
    second = jnp.einsum('bmli,bmlq->liq', pairs[..., 1], partner)
    return first + second


def reference(saved_input, grad_output, legendre, quad_weight, mixing_weight):
    analysis = (legendre.astype(jnp.float32) * quad_weight[None, None, :]).astype(jnp.bfloat16)
    analysis_wide = analysis.astype(jnp.float32)
    spectra = jnp.einsum('mlj,bmjq->bmlq', analysis_wide, saved_input.astype(jnp.float32)).astype(jnp.bfloat16)
    grad_spectra = jnp.einsum('mlj,bmjq->bmlq', legendre.astype(jnp.float32), grad_output.astype(jnp.float32)).astype(jnp.bfloat16)
    batch = saved_input.shape[0]
    spec_wide = spectra.astype(jnp.float32)
    grad_wide = grad_spectra.astype(jnp.float32)
    spec_groups = spec_wide.reshape((N_DP, batch // N_DP) + spec_wide.shape[1:])
    grad_groups = grad_wide.reshape((N_DP, batch // N_DP) + grad_wide.shape[1:])

    def add_group(running, members):
        term = weight_terms(members[0], members[1]) / batch
        rounded = lax.optimization_barrier(term.astype(jnp.bfloat16))
        return running + rounded.astype(jnp.float32), None

    initial = jnp.zeros(mixing_weight.shape, jnp.float32)
    summed, unused = lax.scan(add_group, initial, (spec_groups, grad_groups))
    grad_weight = summed.astype(jnp.bfloat16)

    width = 2 * C // N_CHAN
    partner_wide = partner_of(grad_wide)
    grad_blocks = jnp.moveaxis(grad_wide.reshape(grad_wide.shape[:3] + (N_CHAN, width)), 3, 0)
    partner_blocks = jnp.moveaxis(partner_wide.reshape(partner_wide.shape[:3] + (N_CHAN, width)), 3, 0)
    weight_wide = mixing_weight.astype(jnp.float32)
    weight_blocks = jnp.moveaxis(weight_wide.reshape(weight_wide.shape[:2] + (N_CHAN, width)), 2, 0)

    def add_block(running, members):
        grads_block, partner_block, weights_block = members
        sum_real = jnp.einsum('bmlq,liq->bmli', grads_block, weights_block)
        sum_imag = jnp.einsum('bmlq,liq->bmli', partner_block, weights_block)
        term = jnp.stack([sum_real, sum_imag], axis=-1).reshape(running.shape)
        rounded = lax.optimization_barrier(term.astype(jnp.bfloat16))
        return running + rounded.astype(jnp.float32), None

    start_sum = jnp.zeros(spec_wide.shape, jnp.float32)
    spec_sum, unused_two = lax.scan(add_block, start_sum, (grad_blocks, partner_blocks, weight_blocks))
    grad_spec_in = spec_sum.astype(jnp.bfloat16)
    grad_input = jnp.einsum('mlj,bmlq->bmjq', analysis_wide, grad_spec_in.astype(jnp.float32)).astype(jnp.bfloat16)
    return (grad_weight, grad_input)
```

```python
import jax
import jax.numpy as jnp
from jax import lax
from jax.experimental import pallas as pl
from jax.experimental.pallas import tpu as pltpu
from jax.sharding import PartitionSpec as P

MESH = pl.DeviceIdType.MESH
BF = jnp.bfloat16
F32 = jnp.float32

M, J, Q, LB, MB, CH, NZ = 64, 45, 128, 12, 4, 192, 16
ROWS = NZ * LB * MB
NCHAN, NDP = 8, 4


def iota(shape, dim):
    return lax.broadcasted_iota(jnp.int32, shape, dim)


def dot(a, b, dims=((1,), (0,))):
    return lax.dot_general(a, b, (dims, ((), ())), preferred_element_type=F32)


def one_hot(hit):
    return jnp.where(hit, 1.0, 0.0).astype(BF)


def offset_of(s):
    k = (s + 1) // 2
    far = 8 - k
    return jnp.where(s % 2 == 1, far, NZ - far)


def kernel(
    go, si, leg, quad, w, gw, gi,
    r_syn, r_ana, t_syn, t_ana, t_back, p_in, p_out, p_sort, p_unsort, w2,
    g1s, g1r, s1s, s1r, acc, g2s, g2r, s2s, s2r, gall, sall, ks, kr, b3s, b3r, o4s, o4r,
    g_ss, g_rs, s_ss, s_rs, g2_ss, g2_rs, s2_ss, s2_rs, k_ss, k_rs, d_ss, d_rs, e_ss, e_rs,
    b_ss, b_rs, o_ss, o_rs,
):
    dp, z, ch = lax.axis_index("dp"), lax.axis_index("lat"), lax.axis_index("chan")
    barrier = pltpu.get_barrier_semaphore()

    def greet_z(s, c):
        to = (z + s + 1) % NZ
        pl.semaphore_signal(barrier, inc=1, device_id={"lat": to}, device_id_type=MESH)
        return c

    def greet_plane(s, c):
        other = (dp * NCHAN + ch + s + 1) % (NDP * NCHAN)
        pl.semaphore_signal(
            barrier, inc=1, device_id={"dp": other // NCHAN, "chan": other % NCHAN}, device_id_type=MESH
        )
        return c

    lax.fori_loop(0, NZ - 1, greet_z, 0)
    lax.fori_loop(0, NDP * NCHAN - 1, greet_plane, 0)

    def z_copy(src, dst, ss, rs, to, slot):
        return pltpu.make_async_remote_copy(
            src_ref=src.at[to], dst_ref=dst.at[slot], send_sem=ss.at[to], recv_sem=rs.at[slot],
            device_id={"lat": to}, device_id_type=MESH,
        )

    def z_send(src, dst, ss, rs, first, last, flip=False):
        def step(s, c):
            to = (z + offset_of(NZ - 2 - s if flip else s)) % NZ
            z_copy(src, dst, ss, rs, to, z).start()
            return c

        lax.fori_loop(first, last, step, 0)

    def z_wait_sends(src, dst, ss, rs):
        def step(s, c):
            z_copy(src, dst, ss, rs, (z + s + 1) % NZ, z).wait_send()
            return c

        lax.fori_loop(0, NZ - 1, step, 0)

    def z_wait_recv(src, dst, ss, rs, s):
        frm = (z + NZ - offset_of(s)) % NZ
        z_copy(src, dst, ss, rs, frm, frm).wait_recv()
        return frm

    def z_wait_all(src, dst, ss, rs):
        def step(s, c):
            z_wait_recv(src, dst, ss, rs, s)
            return c

        lax.fori_loop(0, NZ - 1, step, 0)

    for zz in range(4):
        r, c = iota((CH, 16 * J), 0), iota((CH, 16 * J), 1)
        p_in[pl.ds(zz * CH, CH), :] = one_hot((c == (r // 4) * 16 + zz * 4 + r % 4) & (r < MB * J))

    def order_in(x, out):
        def step(g, c):
            rows = x[:, pl.ds(pl.multiple_of(16 * g, 16), 16), :].reshape(16 * J, Q)
            out[pl.ds(4 * g, 4)] = dot(p_in[...], rows).astype(BF).reshape(4, CH, Q)
            return c

        lax.fori_loop(0, 4, step, 0)

    order_in(go, g1s)
    pl.semaphore_wait(barrier, NZ - 1 + NDP * NCHAN - 1)
    z_send(g1s, g1r, g_ss, g_rs, 0, NZ - 1)
    order_in(si, s1s)
    z_send(s1s, s1r, s_ss, s_rs, 0, 8, flip=True)
    g1r[z] = g1s[z]
    s1r[z] = s1s[z]

    zero = jnp.zeros((ROWS, ROWS - 720), BF)
    r_syn[:, 720:] = zero
    r_ana[:, 720:] = zero

    def rows_of(ib, c):
        r = iota((128, ROWS), 0) + ib * 128
        pick = one_hot(iota((128, ROWS), 1) == (r % 4) * (NZ * LB) + r // 4)
        flat = leg[...].reshape(ROWS, 720)
        at = pl.ds(pl.multiple_of(ib * 128, 128), 128)
        syn = dot(pick, flat)
        r_syn[at, :720] = syn.astype(BF)
        r_ana[at, :720] = (syn * quad[...]).astype(BF)
        return c

    lax.fori_loop(0, ROWS // 128, rows_of, 0)

    def window(zz):
        start = jnp.minimum((zz * J) // 128, 4) * 128
        return pl.ds(pl.multiple_of(start, 128), 256), zz * J - start

    def table(src, dst):
        def step(zz, c):
            at, off = window(zz)
            r, k = iota((256, CH), 0), iota((256, CH), 1)
            pick = one_hot((r == off + k // 4) & (k < MB * J))
            full = dot(src[:, at], pick)
            keep = iota((ROWS, CH), 0) % 4 == iota((ROWS, CH), 1) % 4
            dst[zz] = jnp.where(keep, full, 0.0).astype(BF)
            return c

        lax.fori_loop(0, NZ, step, 0)

    table(r_syn, t_syn)

    def sort_block(ib, c):
        at = pl.ds(pl.multiple_of(ib * 128, 128), 128)
        r, k = iota((128, ROWS), 0) + ib * 128, iota((128, ROWS), 1)
        p_sort[at, :] = one_hot(k == ((r % M) // 4) * 48 + (r // M) * 4 + r % 4)
        p_unsort[at, :] = one_hot(r == ((k % M) // 4) * 48 + (k // M) * 4 + k % 4)
        return c

    lax.fori_loop(0, ROWS // 128, sort_block, 0)

    ra, ca = iota((Q, Q), 0), iota((Q, Q), 1)
    swap = jnp.where(ca == ra + 1, 1.0, 0.0) * jnp.where(ra % 2 == 0, 1.0, 0.0)
    swap = (swap - jnp.where(ra == ca + 1, 1.0, 0.0) * jnp.where(ca % 2 == 0, 1.0, 0.0)).astype(BF)
    r2, c2 = iota((256, 256), 0), iota((256, 256), 1)
    weave = one_hot(c2 == (r2 % 2) * 128 + r2 // 2)

    def weave_weight(l, c):
        for k in range(4):
            block = w[l, pl.ds(128 * k, 128), :]
            both = jnp.concatenate([block, dot(block, swap).astype(BF)], axis=0)
            w2[l, pl.ds(256 * k, 256), :] = dot(weave, both).astype(BF)
        return c

    lax.fori_loop(0, LB, weave_weight, 0)
    table(r_ana, t_ana)

    def back_table(zz, c):
        at, off = window(zz)
        r, k = iota((CH, 256), 0), iota((CH, 256), 1)
        pick = one_hot((k == off + r // 4) & (r < MB * J))
        full = dot(pick, r_ana[:, at], ((1,), (1,)))
        keep = iota((CH, ROWS), 0) % 4 == iota((CH, ROWS), 1) % 4
        t_back[zz] = jnp.where(keep, full, 0.0).astype(BF)
        return c

    lax.fori_loop(0, NZ, back_table, 0)

    def legendre_sum(t, send, recv, ss, rs, out, flip=False):
        acc[...] = dot(t[z], recv[z])

        def step(s, c):
            frm = z_wait_recv(send, recv, ss, rs, NZ - 2 - s if flip else s)
            acc[...] += dot(t[frm], recv[frm])
            return c

        lax.fori_loop(0, NZ - 1, step, 0)
        out[...] = acc[...].astype(BF).reshape(NZ, LB * MB, Q)

    legendre_sum(t_syn, g1s, g1r, g_ss, g_rs, g2s)
    z_send(g2s, g2r, g2_ss, g2_rs, 0, NZ - 1)
    z_send(s1s, s1r, s_ss, s_rs, 8, NZ - 1, flip=True)
    g2r[z] = g2s[z]
    z_wait_all(g2s, g2r, g2_ss, g2_rs)
    grads = dot(p_sort[...], g2r[...].reshape(ROWS, Q)).astype(BF).reshape(LB, M, Q)
    gall[dp] = grads

    def mix(l, c):
        full = dot(gall[dp, l], w2[l], ((1,), (1,))).astype(BF)
        for k in range(NCHAN):
            ks[k, l] = full[:, 128 * k : 128 * k + 128]
        return c

    lax.fori_loop(0, LB, mix, 0)

    def k_copy(to, slot):
        return pltpu.make_async_remote_copy(
            src_ref=ks.at[to], dst_ref=kr.at[slot], send_sem=k_ss.at[to], recv_sem=k_rs.at[slot],
            device_id={"chan": to}, device_id_type=MESH,
        )

    def k_send(s, c):
        k_copy((ch + s + 1) % NCHAN, ch).start()
        return c

    lax.fori_loop(0, NCHAN - 1, k_send, 0)

    def d_copy(to, slot):
        return pltpu.make_async_remote_copy(
            src_ref=gall.at[dp], dst_ref=gall.at[slot], send_sem=d_ss.at[to], recv_sem=d_rs.at[slot],
            device_id={"dp": to}, device_id_type=MESH,
        )

    def d_send(s, c):
        d_copy((dp + s + 1) % NDP, dp).start()
        return c

    lax.fori_loop(0, NDP - 1, d_send, 0)
    kr[ch] = ks[ch]

    legendre_sum(t_ana, s1s, s1r, s_ss, s_rs, s2s, flip=True)
    z_send(s2s, s2r, s2_ss, s2_rs, 0, NZ - 1)
    s2r[z] = s2s[z]

    def k_wait(s, c):
        frm = (ch + s + 1) % NCHAN
        k_copy(frm, frm).wait_recv()
        return c

    lax.fori_loop(0, NCHAN - 1, k_wait, 0)

    def sum_terms(l, c):
        total = kr[0, l].astype(F32)
        for k in range(1, NCHAN):
            total = total + kr[k, l].astype(F32)
        kr[0, l] = total.astype(BF)
        return c

    lax.fori_loop(0, LB, sum_terms, 0)
    b3s[...] = dot(p_unsort[...], kr[0].reshape(ROWS, Q)).astype(BF).reshape(NZ, LB * MB, Q)
    z_send(b3s, b3r, b_ss, b_rs, 0, NZ - 1)
    b3r[z] = b3s[z]

    home, half = ch // 2, ch % 2
    z_wait_all(s2s, s2r, s2_ss, s2_rs)
    mine = sall.at[dp, half]
    spectra = dot(p_sort[...], s2r[...].reshape(ROWS, Q)).astype(BF).reshape(LB, M, Q)
    s2all = ks.at[ch]
    s2all[...] = spectra

    def e_copy(to, b, h):
        return pltpu.make_async_remote_copy(
            src_ref=ks.at[ch], dst_ref=sall.at[b, h], send_sem=e_ss.at[to], recv_sem=e_rs.at[b, h],
            device_id={"dp": home, "chan": to}, device_id_type=MESH,
        )

    def e_send(s, c):
        to = (ch + s) % NCHAN

        @pl.when((to != ch) | (home != dp))
        def _():
            e_copy(to, dp, half).start()

        return c

    lax.fori_loop(0, NCHAN, e_send, 0)

    @pl.when(home == dp)
    def _():
        mine[...] = spectra

    z_wait_all(b3s, b3r, b_ss, b_rs)

    def back(s, c):
        to = (z + offset_of(s)) % NZ
        o4s[to] = dot(t_back[to], b3r[...].reshape(ROWS, Q)).astype(BF)
        z_copy(o4s, o4r, o_ss, o_rs, to, z).start()
        return c

    lax.fori_loop(0, NZ - 1, back, 0)
    o4r[z] = dot(t_back[z], b3r[...].reshape(ROWS, Q)).astype(BF)
    for zz in range(4):
        r, c = iota((16 * J, CH), 0), iota((16 * J, CH), 1)
        p_out[:, pl.ds(zz * CH, CH)] = one_hot((r == (c // 4) * 16 + zz * 4 + c % 4) & (c < MB * J))

    def d_wait(s, c):
        frm = (dp + s + 1) % NDP
        d_copy(frm, frm).wait_recv()
        return c

    lax.fori_loop(0, NDP - 1, d_wait, 0)
    for b in range(NDP):
        for h in range(2):

            @pl.when((b != dp) | (2 * dp + h != ch))
            def _():
                e_copy(ch, b, h).wait_recv()

    apart = one_hot(r2 == 2 * (c2 % 128) + c2 // 128)
    partner_of = (-swap.astype(F32)).astype(BF)

    def weight(l, c):
        left, right = [], []
        for b in range(NDP):
            both = jnp.concatenate([sall[b, 0, l], sall[b, 1, l]], axis=1)
            parts = dot(both, apart).astype(BF)
            left += [parts[:, :128], parts[:, 128:]]
            g = gall[b, l]
            right += [g, dot(g, partner_of).astype(BF)]
        total = dot(jnp.concatenate(left, axis=0), jnp.concatenate(right, axis=0), ((0,), (0,)))
        gw[l] = (total * 0.25).astype(BF)
        return c

    lax.fori_loop(0, LB, weight, 0)

    z_wait_all(o4s, o4r, o_ss, o_rs)

    def order_out(g, c):
        rows = o4r[pl.ds(4 * g, 4)].reshape(4 * CH, Q)
        out = dot(p_out[...], rows).astype(BF).reshape(J, 16, Q)
        gi[:, pl.ds(pl.multiple_of(16 * g, 16), 16), :] = out
        return c

    lax.fori_loop(0, 4, order_out, 0)

    for args in (
        (g1s, g1r, g_ss, g_rs), (s1s, s1r, s_ss, s_rs), (g2s, g2r, g2_ss, g2_rs),
        (s2s, s2r, s2_ss, s2_rs), (b3s, b3r, b_ss, b_rs), (o4s, o4r, o_ss, o_rs),
    ):
        z_wait_sends(*args)

    def k_done(s, c):
        k_copy((ch + s + 1) % NCHAN, ch).wait_send()
        return c

    lax.fori_loop(0, NCHAN - 1, k_done, 0)

    def d_done(s, c):
        d_copy((dp + s + 1) % NDP, dp).wait_send()
        return c

    lax.fori_loop(0, NDP - 1, d_done, 0)

    def e_done(s, c):
        to = (ch + s) % NCHAN

        @pl.when((to != ch) | (home != dp))
        def _():
            e_copy(to, dp, half).wait_send()

        return c

    lax.fori_loop(0, NCHAN, e_done, 0)


def on_device(saved_input, grad_output, legendre, quad_weight, mixing_weight):
    go = grad_output[0].transpose(1, 0, 2)
    si = saved_input[0].transpose(1, 0, 2)
    vmem = pl.BlockSpec(memory_space=pltpu.VMEM)
    dma = pltpu.SemaphoreType.DMA
    gw, gi = pl.pallas_call(
        kernel,
        out_shape=(
            jax.ShapeDtypeStruct((LB, Q, Q), BF),
            jax.ShapeDtypeStruct((J, M, Q), BF),
        ),
        in_specs=[vmem] * 5,
        out_specs=(vmem, vmem),
        scratch_shapes=[
            pltpu.VMEM((ROWS, ROWS), BF), pltpu.VMEM((ROWS, ROWS), BF),
            pltpu.VMEM((NZ, ROWS, CH), BF), pltpu.VMEM((NZ, ROWS, CH), BF),
            pltpu.VMEM((NZ, CH, ROWS), BF),
            pltpu.VMEM((4 * CH, 16 * J), BF), pltpu.VMEM((16 * J, 4 * CH), BF),
            pltpu.VMEM((ROWS, ROWS), BF), pltpu.VMEM((ROWS, ROWS), BF),
            pltpu.VMEM((LB, 1024, Q), BF),
            pltpu.VMEM((NZ, CH, Q), BF), pltpu.VMEM((NZ, CH, Q), BF),
            pltpu.VMEM((NZ, CH, Q), BF), pltpu.VMEM((NZ, CH, Q), BF),
            pltpu.VMEM((ROWS, Q), F32),
            pltpu.VMEM((NZ, LB * MB, Q), BF), pltpu.VMEM((NZ, LB * MB, Q), BF),
            pltpu.VMEM((NZ, LB * MB, Q), BF), pltpu.VMEM((NZ, LB * MB, Q), BF),
            pltpu.VMEM((NDP, LB, M, Q), BF), pltpu.VMEM((NDP, 2, LB, M, Q), BF),
            pltpu.VMEM((NCHAN, LB, M, Q), BF), pltpu.VMEM((NCHAN, LB, M, Q), BF),
            pltpu.VMEM((NZ, LB * MB, Q), BF), pltpu.VMEM((NZ, LB * MB, Q), BF),
            pltpu.VMEM((NZ, CH, Q), BF), pltpu.VMEM((NZ, CH, Q), BF),
            dma((NZ,)), dma((NZ,)), dma((NZ,)), dma((NZ,)), dma((NZ,)), dma((NZ,)),
            dma((NZ,)), dma((NZ,)), dma((NCHAN,)), dma((NCHAN,)), dma((NDP,)), dma((NDP,)),
            dma((NCHAN,)), dma((NDP, 2)), dma((NZ,)), dma((NZ,)), dma((NZ,)), dma((NZ,)),
        ],
        compiler_params=pltpu.CompilerParams(
            collective_id=0, has_side_effects=True, vmem_limit_bytes=63_000_000
        ),
    )(go, si, legendre, quad_weight[None, :], mixing_weight)
    return gw, gi.transpose(1, 0, 2)[None]


def solution(mesh):
    in_specs = (
        P("dp", None, "lat", "chan"),
        P("dp", None, "lat", "chan"),
        P("lat", None, None),
        P(),
        P("lat", None, "chan"),
    )
    out_specs = (P("lat", "dp", "chan"), P("dp", None, "lat", "chan"))
    return jax.shard_map(
        on_device, mesh=mesh, in_specs=in_specs, out_specs=out_specs, check_vma=False
    )
```

```python
import jax
import jax.numpy as jnp
from jax import lax
from jax.experimental import pallas as pl
from jax.experimental.pallas import tpu as pltpu
from jax.sharding import PartitionSpec as P

MESH = pl.DeviceIdType.MESH
BF = jnp.bfloat16
F32 = jnp.float32

M, J, Q, LB, MB, CH, NZ = 64, 45, 128, 12, 4, 192, 16
ROWS = NZ * LB * MB
NCHAN, NDP = 8, 4
SHARES = 24


def iota(shape, dim):
    return lax.broadcasted_iota(jnp.int32, shape, dim)


def dot(a, b, dims=((1,), (0,))):
    return lax.dot_general(a, b, (dims, ((), ())), preferred_element_type=F32)


def one_hot(hit):
    return jnp.where(hit, 1.0, 0.0).astype(BF)


def offset_of(s):
    k = (s + 1) // 2
    far = 8 - k
    return jnp.where(s % 2 == 1, far, NZ - far)


def kernel(
    go, si, leg, quad, w, gw, gi,
    r_syn, r_ana, t_syn, t_ana, p_in, p_sort, p_unsort, w2,
    g1s, g1r, s1s, s1r, acc, g2s, g2r, s2s, s2r, gall, sall, ks, kr,
    xa, tsend, trecv, tall, xr, t_back, ag, oacc,
    g_ss, g_rs, s_ss, s_rs, g2_ss, g2_rs, s2_ss, s2_rs, k_ss, k_rs, d_ss, d_rs, e_ss, e_rs,
    t_ss, t_rs, a_ss, a_rs, r_ss, r_rs,
):
    dp, z, ch = lax.axis_index("dp"), lax.axis_index("lat"), lax.axis_index("chan")
    barrier = pltpu.get_barrier_semaphore()

    def greet_z(s, c):
        to = (z + s + 1) % NZ
        pl.semaphore_signal(barrier, inc=1, device_id={"lat": to}, device_id_type=MESH)
        return c

    def greet_plane(s, c):
        other = (dp * NCHAN + ch + s + 1) % (NDP * NCHAN)
        pl.semaphore_signal(
            barrier, inc=1, device_id={"dp": other // NCHAN, "chan": other % NCHAN}, device_id_type=MESH
        )
        return c

    lax.fori_loop(0, NZ - 1, greet_z, 0)
    lax.fori_loop(0, NDP * NCHAN - 1, greet_plane, 0)

    def z_copy(src, dst, ss, rs, to, slot):
        return pltpu.make_async_remote_copy(
            src_ref=src.at[to], dst_ref=dst.at[slot], send_sem=ss.at[to], recv_sem=rs.at[slot],
            device_id={"lat": to}, device_id_type=MESH,
        )

    def z_send(src, dst, ss, rs, first, last, flip=False):
        def step(s, c):
            to = (z + offset_of(NZ - 2 - s if flip else s)) % NZ
            z_copy(src, dst, ss, rs, to, z).start()
            return c

        lax.fori_loop(first, last, step, 0)

    def z_wait_sends(src, dst, ss, rs):
        def step(s, c):
            z_copy(src, dst, ss, rs, (z + s + 1) % NZ, z).wait_send()
            return c

        lax.fori_loop(0, NZ - 1, step, 0)

    def z_wait_recv(src, dst, ss, rs, s):
        frm = (z + NZ - offset_of(s)) % NZ
        z_copy(src, dst, ss, rs, frm, frm).wait_recv()
        return frm

    def z_wait_all(src, dst, ss, rs):
        def step(s, c):
            z_wait_recv(src, dst, ss, rs, s)
            return c

        lax.fori_loop(0, NZ - 1, step, 0)

    for zz in range(4):
        r, c = iota((CH, 16 * J), 0), iota((CH, 16 * J), 1)
        p_in[pl.ds(zz * CH, CH), :] = one_hot((c == (r // 4) * 16 + zz * 4 + r % 4) & (r < MB * J))

    def order_in(x, out):
        def step(g, c):
            rows = x[:, pl.ds(pl.multiple_of(16 * g, 16), 16), :].reshape(16 * J, Q)
            out[pl.ds(4 * g, 4)] = dot(p_in[...], rows).astype(BF).reshape(4, CH, Q)
            return c

        lax.fori_loop(0, 4, step, 0)

    order_in(go, g1s)
    pl.semaphore_wait(barrier, NZ - 1 + NDP * NCHAN - 1)
    z_send(g1s, g1r, g_ss, g_rs, 0, 3)

    me = dp * NCHAN + ch
    shares = me < SHARES
    group, pair = jnp.minimum(me // 2, SHARES // 2 - 1), me % 2
    for h in range(2):
        part = leg[2 * pair + h, pl.ds(pl.multiple_of(16 * group, 16), 16), :].astype(F32)
        xa[h, :, 720:] = jnp.zeros((16, ROWS - 720), BF)
        xa[h, :, :720] = (part * quad[...]).astype(BF)

    def window(zz):
        start = jnp.minimum((zz * J) // 128, 4) * 128
        return pl.ds(pl.multiple_of(start, 128), 256), zz * J - start

    def cut(zz, c):
        at, off = window(zz)
        r, k = iota((512, 128), 0), iota((512, 128), 1)
        pick = one_hot((r % 256 == off + k % 64) & (r // 256 == k // 64) & (k % 64 < J))
        both = jnp.concatenate([xa[0, :, at], xa[1, :, at]], axis=1)
        tsend[zz] = dot(both, pick).astype(BF)
        return c

    lax.fori_loop(0, NZ, cut, 0)

    @pl.when(shares)
    def _():
        z_send(tsend, trecv, t_ss, t_rs, 0, NZ - 1)

    trecv[z] = tsend[z]
    z_send(g1s, g1r, g_ss, g_rs, 3, NZ - 1)
    order_in(si, s1s)
    z_send(s1s, s1r, s_ss, s_rs, 0, 8, flip=True)
    g1r[z] = g1s[z]
    s1r[z] = s1s[z]

    zero = jnp.zeros((ROWS, ROWS - 720), BF)
    r_syn[:, 720:] = zero
    r_ana[:, 720:] = zero

    def rows_of(ib, c):
        r = iota((128, ROWS), 0) + ib * 128
        pick = one_hot(iota((128, ROWS), 1) == (r % 4) * (NZ * LB) + r // 4)
        flat = leg[...].reshape(ROWS, 720)
        at = pl.ds(pl.multiple_of(ib * 128, 128), 128)
        syn = dot(pick, flat)
        r_syn[at, :720] = syn.astype(BF)
        r_ana[at, :720] = (syn * quad[...]).astype(BF)
        return c

    lax.fori_loop(0, ROWS // 128, rows_of, 0)

    def table(src, dst):
        def step(zz, c):
            at, off = window(zz)
            r, k = iota((256, CH), 0), iota((256, CH), 1)
            pick = one_hot((r == off + k // 4) & (k < MB * J))
            full = dot(src[:, at], pick)
            keep = iota((ROWS, CH), 0) % 4 == iota((ROWS, CH), 1) % 4
            dst[zz] = jnp.where(keep, full, 0.0).astype(BF)
            return c

        lax.fori_loop(0, NZ, step, 0)

    table(r_syn, t_syn)

    def sort_block(ib, c):
        at = pl.ds(pl.multiple_of(ib * 128, 128), 128)
        r, k = iota((128, ROWS), 0) + ib * 128, iota((128, ROWS), 1)
        p_sort[at, :] = one_hot(k == ((r % M) // 4) * 48 + (r // M) * 4 + r % 4)
        p_unsort[at, :] = one_hot(k == ((r % 96) // 8) * M + (r // 96) * 8 + r % 8)
        return c

    lax.fori_loop(0, ROWS // 128, sort_block, 0)

    ra, ca = iota((Q, Q), 0), iota((Q, Q), 1)
    swap = jnp.where(ca == ra + 1, 1.0, 0.0) * jnp.where(ra % 2 == 0, 1.0, 0.0)
    swap = (swap - jnp.where(ra == ca + 1, 1.0, 0.0) * jnp.where(ca % 2 == 0, 1.0, 0.0)).astype(BF)
    r2, c2 = iota((256, 256), 0), iota((256, 256), 1)
    weave = one_hot(c2 == (r2 % 2) * 128 + r2 // 2)

    def weave_weight(l, c):
        for k in range(4):
            block = w[l, pl.ds(128 * k, 128), :]
            both = jnp.concatenate([block, dot(block, swap).astype(BF)], axis=0)
            w2[l, pl.ds(256 * k, 256), :] = dot(weave, both).astype(BF)
        return c

    lax.fori_loop(0, LB, weave_weight, 0)

    def a_copy(to, frm):
        return pltpu.make_async_remote_copy(
            src_ref=trecv, dst_ref=tall.at[frm], send_sem=a_ss.at[to], recv_sem=a_rs.at[frm],
            device_id={"dp": to // NCHAN, "chan": to % NCHAN}, device_id_type=MESH,
        )

    @pl.when(shares)
    def _():
        z_wait_all(tsend, trecv, t_ss, t_rs)

        def a_send(s, c):
            a_copy((me + s + 1) % (NDP * NCHAN), me).start()
            return c

        lax.fori_loop(0, NDP * NCHAN - 1, a_send, 0)
        tall[me] = trecv[...]

    table(r_ana, t_ana)

    def legendre_sum(t, send, recv, ss, rs, out, flip=False):
        acc[...] = dot(t[z], recv[z])

        def step(s, c):
            frm = z_wait_recv(send, recv, ss, rs, NZ - 2 - s if flip else s)
            acc[...] += dot(t[frm], recv[frm])
            return c

        lax.fori_loop(0, NZ - 1, step, 0)
        out[...] = acc[...].astype(BF).reshape(NZ, LB * MB, Q)

    legendre_sum(t_syn, g1s, g1r, g_ss, g_rs, g2s)
    z_send(g2s, g2r, g2_ss, g2_rs, 0, NZ - 1)
    z_send(s1s, s1r, s_ss, s_rs, 8, NZ - 1, flip=True)
    g2r[z] = g2s[z]
    z_wait_all(g2s, g2r, g2_ss, g2_rs)
    grads = dot(p_sort[...], g2r[...].reshape(ROWS, Q)).astype(BF).reshape(LB, M, Q)
    gall[dp] = grads

    def mix(l, c):
        full = dot(gall[dp, l], w2[l], ((1,), (1,))).astype(BF)
        for k in range(NCHAN):
            ks[k, l] = full[:, 128 * k : 128 * k + 128]
        return c

    lax.fori_loop(0, LB, mix, 0)

    def k_copy(to, slot):
        return pltpu.make_async_remote_copy(
            src_ref=ks.at[to], dst_ref=kr.at[slot], send_sem=k_ss.at[to], recv_sem=k_rs.at[slot],
            device_id={"chan": to}, device_id_type=MESH,
        )

    def k_send(s, c):
        k_copy((ch + s + 1) % NCHAN, ch).start()
        return c

    lax.fori_loop(0, NCHAN - 1, k_send, 0)

    def d_copy(to, slot):
        return pltpu.make_async_remote_copy(
            src_ref=gall.at[dp], dst_ref=gall.at[slot], send_sem=d_ss.at[to], recv_sem=d_rs.at[slot],
            device_id={"dp": to}, device_id_type=MESH,
        )

    def d_send(s, c):
        d_copy((dp + s + 1) % NDP, dp).start()
        return c

    lax.fori_loop(0, NDP - 1, d_send, 0)
    kr[ch] = ks[ch]

    def a_wait(s, c):
        @pl.when(s != me)
        def _():
            a_copy(s, s).wait_recv()

        return c

    lax.fori_loop(0, SHARES, a_wait, 0)
    rx, cx = iota((128, 64), 0), iota((128, 64), 1)
    spread = one_hot(cx == ((rx % 8) // 2) * 16 + rx // 8)

    def by_degree(i, c):
        g, lg = i % 8, i // 8
        tiles = [tall[2 * lg + t % 2, 2 * g + t // 2] for t in range(4)]
        at = pl.ds(pl.multiple_of(lg * 128, 128), 128)
        xr[g, at, :] = dot(spread, jnp.concatenate(tiles, axis=0)).astype(BF)
        return c

    lax.fori_loop(0, 96, by_degree, 0)

    def back_table(i, c):
        g, o = i % 8, i // 8
        r, k = iota((8 * J, 128), 0), iota((8 * J, 128), 1)
        pick = one_hot(k == (r % 2) * 64 + r // 8)
        full = dot(pick, xr[g, pl.ds(pl.multiple_of(o * 96, 32), 96), :], ((1,), (1,)))
        keep = iota((8 * J, 96), 0) % 8 == iota((8 * J, 96), 1) % 8
        t_back[o, g] = jnp.where(keep, full, 0.0).astype(BF)
        return c

    lax.fori_loop(0, 8 * NZ, back_table, 0)

    legendre_sum(t_ana, s1s, s1r, s_ss, s_rs, s2s, flip=True)
    z_send(s2s, s2r, s2_ss, s2_rs, 0, NZ - 1)
    s2r[z] = s2s[z]

    def k_wait(s, c):
        frm = (ch + s + 1) % NCHAN
        k_copy(frm, frm).wait_recv()
        return c

    lax.fori_loop(0, NCHAN - 1, k_wait, 0)

    def sum_terms(l, c):
        total = kr[0, l].astype(F32)
        for k in range(1, NCHAN):
            total = total + kr[k, l].astype(F32)
        kr[0, l] = total.astype(BF)
        return c

    lax.fori_loop(0, LB, sum_terms, 0)
    ag[z] = dot(p_unsort[...], kr[0].reshape(ROWS, Q)).astype(BF).reshape(8, 96, Q)

    def r_copy(side, hop, part, origin):
        to = (z + (1 if side == 0 else NZ - 1)) % NZ
        at = pl.ds(2 * part, 2)
        return pltpu.make_async_remote_copy(
            src_ref=ag.at[origin, at], dst_ref=ag.at[origin, at],
            send_sem=r_ss.at[side, hop, part], recv_sem=r_rs.at[side, hop, part],
            device_id={"lat": to}, device_id_type=MESH,
        )

    for part in range(4):
        for side in range(2):
            r_copy(side, 0, part, z).start()

    home, half = ch // 2, ch % 2
    z_wait_all(s2s, s2r, s2_ss, s2_rs)
    mine = sall.at[dp, half]
    spectra = dot(p_sort[...], s2r[...].reshape(ROWS, Q)).astype(BF).reshape(LB, M, Q)
    s2all = ks.at[ch]
    s2all[...] = spectra

    def e_copy(to, b, h):
        return pltpu.make_async_remote_copy(
            src_ref=ks.at[ch], dst_ref=sall.at[b, h], send_sem=e_ss.at[to], recv_sem=e_rs.at[b, h],
            device_id={"dp": home, "chan": to}, device_id_type=MESH,
        )

    def e_send(s, c):
        to = (ch + s) % NCHAN

        @pl.when((to != ch) | (home != dp))
        def _():
            e_copy(to, dp, half).start()

        return c

    lax.fori_loop(0, NCHAN, e_send, 0)

    @pl.when(home == dp)
    def _():
        mine[...] = spectra

    for g in range(8):
        oacc[g] = dot(t_back[z, g], ag[z, g])

    def hop_in(k, c):
        left, right = (z + NZ - k) % NZ, (z + k) % NZ
        for part in range(4):
            for side, origin in ((0, left), (1, right)):
                r_copy(side, k - 1, part, origin).wait_recv()
                if part // 2 == side:
                    r_copy(side, k, part, origin).start()
                else:

                    @pl.when(k < NZ // 2 - 1)
                    def _():
                        r_copy(side, k, part, origin).start()

            for g in (2 * part, 2 * part + 1):
                oacc[g] += dot(t_back[left, g], ag[left, g]) + dot(t_back[right, g], ag[right, g])
        return c

    lax.fori_loop(1, NZ // 2, hop_in, 0)

    def d_wait(s, c):
        frm = (dp + s + 1) % NDP
        d_copy(frm, frm).wait_recv()
        return c

    lax.fori_loop(0, NDP - 1, d_wait, 0)
    for b in range(NDP):
        for h in range(2):

            @pl.when((b != dp) | (2 * dp + h != ch))
            def _():
                e_copy(ch, b, h).wait_recv()

    apart = one_hot(r2 == 2 * (c2 % 128) + c2 // 128)
    partner_of = (-swap.astype(F32)).astype(BF)

    def weight(l, c):
        left, right = [], []
        for b in range(NDP):
            both = jnp.concatenate([sall[b, 0, l], sall[b, 1, l]], axis=1)
            parts = dot(both, apart).astype(BF)
            left += [parts[:, :128], parts[:, 128:]]
            g = gall[b, l]
            right += [g, dot(g, partner_of).astype(BF)]
        total = dot(jnp.concatenate(left, axis=0), jnp.concatenate(right, axis=0), ((0,), (0,)))
        gw[l] = (total * 0.25).astype(BF)
        return c

    lax.fori_loop(0, LB, weight, 0)

    across = (z + NZ // 2) % NZ
    for part in range(4):
        r_copy(part // 2, NZ // 2 - 1, part, across).wait_recv()
        halves = []
        for g in (2 * part, 2 * part + 1):
            halves.append((oacc[g] + dot(t_back[across, g], ag[across, g])).reshape(J, 8, Q))
        gi[:, pl.ds(16 * part, 16), :] = jnp.concatenate(halves, axis=1).astype(BF)

    for args in (
        (g1s, g1r, g_ss, g_rs), (s1s, s1r, s_ss, s_rs), (g2s, g2r, g2_ss, g2_rs),
        (s2s, s2r, s2_ss, s2_rs),
    ):
        z_wait_sends(*args)

    @pl.when(shares)
    def _():
        z_wait_sends(tsend, trecv, t_ss, t_rs)

        def a_done(s, c):
            a_copy((me + s + 1) % (NDP * NCHAN), me).wait_send()
            return c

        lax.fori_loop(0, NDP * NCHAN - 1, a_done, 0)

    def r_done(k, c):
        for part in range(4):
            for side in range(2):
                r_copy(side, k, part, z).wait_send()
        return c

    lax.fori_loop(0, NZ // 2 - 1, r_done, 0)
    for part in range(4):
        r_copy(part // 2, NZ // 2 - 1, part, z).wait_send()

    def k_done(s, c):
        k_copy((ch + s + 1) % NCHAN, ch).wait_send()
        return c

    lax.fori_loop(0, NCHAN - 1, k_done, 0)

    def d_done(s, c):
        d_copy((dp + s + 1) % NDP, dp).wait_send()
        return c

    lax.fori_loop(0, NDP - 1, d_done, 0)

    def e_done(s, c):
        to = (ch + s) % NCHAN

        @pl.when((to != ch) | (home != dp))
        def _():
            e_copy(to, dp, half).wait_send()

        return c

    lax.fori_loop(0, NCHAN, e_done, 0)


def on_device(saved_input, grad_output, legendre, quad_weight, mixing_weight):
    go = grad_output[0].transpose(1, 0, 2)
    si = saved_input[0].transpose(1, 0, 2)
    vmem = pl.BlockSpec(memory_space=pltpu.VMEM)
    dma = pltpu.SemaphoreType.DMA
    gw, gi = pl.pallas_call(
        kernel,
        out_shape=(
            jax.ShapeDtypeStruct((LB, Q, Q), BF),
            jax.ShapeDtypeStruct((J, M, Q), BF),
        ),
        in_specs=[vmem] * 5,
        out_specs=(vmem, vmem),
        scratch_shapes=[
            pltpu.VMEM((ROWS, ROWS), BF), pltpu.VMEM((ROWS, ROWS), BF),
            pltpu.VMEM((NZ, ROWS, CH), BF), pltpu.VMEM((NZ, ROWS, CH), BF),
            pltpu.VMEM((4 * CH, 16 * J), BF),
            pltpu.VMEM((ROWS, ROWS), BF), pltpu.VMEM((ROWS, ROWS), BF),
            pltpu.VMEM((LB, 1024, Q), BF),
            pltpu.VMEM((NZ, CH, Q), BF), pltpu.VMEM((NZ, CH, Q), BF),
            pltpu.VMEM((NZ, CH, Q), BF), pltpu.VMEM((NZ, CH, Q), BF),
            pltpu.VMEM((ROWS, Q), F32),
            pltpu.VMEM((NZ, LB * MB, Q), BF), pltpu.VMEM((NZ, LB * MB, Q), BF),
            pltpu.VMEM((NZ, LB * MB, Q), BF), pltpu.VMEM((NZ, LB * MB, Q), BF),
            pltpu.VMEM((NDP, LB, M, Q), BF), pltpu.VMEM((NDP, 2, LB, M, Q), BF),
            pltpu.VMEM((NCHAN, LB, M, Q), BF), pltpu.VMEM((NCHAN, LB, M, Q), BF),
            pltpu.VMEM((2, 16, ROWS), BF), pltpu.VMEM((NZ, 16, 128), BF), pltpu.VMEM((NZ, 16, 128), BF),
            pltpu.VMEM((SHARES, NZ, 16, 128), BF), pltpu.VMEM((8, 8 * CH, 128), BF),
            pltpu.VMEM((NZ, 8, 8 * J, 96), BF), pltpu.VMEM((NZ, 8, 96, Q), BF),
            pltpu.VMEM((8, 8 * J, Q), F32),
            dma((NZ,)), dma((NZ,)), dma((NZ,)), dma((NZ,)), dma((NZ,)), dma((NZ,)),
            dma((NZ,)), dma((NZ,)), dma((NCHAN,)), dma((NCHAN,)), dma((NDP,)), dma((NDP,)),
            dma((NCHAN,)), dma((NDP, 2)), dma((NZ,)), dma((NZ,)),
            dma((NDP * NCHAN,)), dma((SHARES,)), dma((2, NZ // 2, 4)), dma((2, NZ // 2, 4)),
        ],
        compiler_params=pltpu.CompilerParams(
            collective_id=0, has_side_effects=True, vmem_limit_bytes=63_000_000
        ),
    )(go, si, legendre, quad_weight[None, :], mixing_weight)
    return gw, gi.transpose(1, 0, 2)[None]


def solution(mesh):
    in_specs = (
        P("dp", None, "lat", "chan"),
        P("dp", None, "lat", "chan"),
        P("lat", None, None),
        P(),
        P("lat", None, "chan"),
    )
    out_specs = (P("lat", "dp", "chan"), P("dp", None, "lat", "chan"))
    return jax.shard_map(
        on_device, mesh=mesh, in_specs=in_specs, out_specs=out_specs, check_vma=False
    )
```

```python
import jax
import jax.numpy as jnp
from jax import lax
from jax.experimental import pallas as pl
from jax.experimental.pallas import tpu as pltpu
from jax.sharding import PartitionSpec as P

MESH = pl.DeviceIdType.MESH
BF = jnp.bfloat16
F32 = jnp.float32

M, J, Q, LB, MB, CH, NZ = 64, 45, 128, 12, 4, 192, 16
ROWS = NZ * LB * MB
NCHAN, NDP = 8, 4
SHARES = 24


def iota(shape, dim):
    return lax.broadcasted_iota(jnp.int32, shape, dim)


def dot(a, b, dims=((1,), (0,))):
    return lax.dot_general(a, b, (dims, ((), ())), preferred_element_type=F32)


def one_hot(hit):
    return jnp.where(hit, 1.0, 0.0).astype(BF)


def offset_of(s):
    k = (s + 1) // 2
    far = 8 - k
    return jnp.where(s % 2 == 1, far, NZ - far)


def kernel(
    go, si, leg, quad, w, gw, gi,
    r_syn, t_syn, p_in, p_sort, p_unsort, p_merge, w2,
    g1s, g1r, acc, g2s, g2r, gall, sall, ks, kr,
    xa, tsend, trecv, tall, xr, e_col, e_row, keep_f, keep_b, x8, t_f, own, part_r, t_b, ag, oacc,
    g_ss, g_rs, g2_ss, g2_rs, k_ss, k_rs, d_ss, d_rs, e_ss, e_rs,
    t_ss, t_rs, a_ss, a_rs, p_ss, p_rs, r_ss, r_rs,
):
    dp, z, ch = lax.axis_index("dp"), lax.axis_index("lat"), lax.axis_index("chan")
    barrier = pltpu.get_barrier_semaphore()

    def greet_z(s, c):
        to = (z + s + 1) % NZ
        pl.semaphore_signal(barrier, inc=1, device_id={"lat": to}, device_id_type=MESH)
        return c

    def greet_plane(s, c):
        other = (dp * NCHAN + ch + s + 1) % (NDP * NCHAN)
        pl.semaphore_signal(
            barrier, inc=1, device_id={"dp": other // NCHAN, "chan": other % NCHAN}, device_id_type=MESH
        )
        return c

    lax.fori_loop(0, NZ - 1, greet_z, 0)
    lax.fori_loop(0, NDP * NCHAN - 1, greet_plane, 0)

    def z_copy(src, dst, ss, rs, to, slot):
        return pltpu.make_async_remote_copy(
            src_ref=src.at[to], dst_ref=dst.at[slot], send_sem=ss.at[to], recv_sem=rs.at[slot],
            device_id={"lat": to}, device_id_type=MESH,
        )

    def z_send(src, dst, ss, rs, first, last, flip=False):
        def step(s, c):
            to = (z + offset_of(NZ - 2 - s if flip else s)) % NZ
            z_copy(src, dst, ss, rs, to, z).start()
            return c

        lax.fori_loop(first, last, step, 0)

    def z_wait_sends(src, dst, ss, rs):
        def step(s, c):
            z_copy(src, dst, ss, rs, (z + s + 1) % NZ, z).wait_send()
            return c

        lax.fori_loop(0, NZ - 1, step, 0)

    def z_wait_recv(src, dst, ss, rs, s):
        frm = (z + NZ - offset_of(s)) % NZ
        z_copy(src, dst, ss, rs, frm, frm).wait_recv()
        return frm

    def z_wait_all(src, dst, ss, rs):
        def step(s, c):
            z_wait_recv(src, dst, ss, rs, s)
            return c

        lax.fori_loop(0, NZ - 1, step, 0)

    for zz in range(4):
        r, c = iota((CH, 16 * J), 0), iota((CH, 16 * J), 1)
        p_in[pl.ds(zz * CH, CH), :] = one_hot((c == (r // 4) * 16 + zz * 4 + r % 4) & (r < MB * J))

    def order_in(x, out):
        def step(g, c):
            rows = x[:, pl.ds(pl.multiple_of(16 * g, 16), 16), :].reshape(16 * J, Q)
            out[pl.ds(4 * g, 4)] = dot(p_in[...], rows).astype(BF).reshape(4, CH, Q)
            return c

        lax.fori_loop(0, 4, step, 0)

    me = dp * NCHAN + ch
    shares = me < SHARES
    group, pair = jnp.minimum(me // 2, SHARES // 2 - 1), me % 2
    for h in range(2):
        rows = leg[2 * pair + h, pl.ds(pl.multiple_of(16 * group, 16), 16), :].astype(F32)
        xa[h, :, 720:] = jnp.zeros((16, ROWS - 720), BF)
        xa[h, :, :720] = (rows * quad[...].reshape(1, 720)).astype(BF)

    def window(zz):
        start = jnp.minimum((zz * J) // 128, 4) * 128
        return pl.ds(pl.multiple_of(start, 128), 256), zz * J - start

    def cut(i, c):
        for u in range(4):
            zz = 4 * i + u
            at, off = window(zz)
            r, k = iota((512, 128), 0), iota((512, 128), 1)
            pick = one_hot((r % 256 == off + k % 64) & (r // 256 == k // 64) & (k % 64 < J))
            both = jnp.concatenate([xa[0, :, at], xa[1, :, at]], axis=1)
            tsend[zz] = dot(both, pick).astype(BF)
        return c

    lax.fori_loop(0, NZ // 4, cut, 0)
    order_in(go, g1s)
    pl.semaphore_wait(barrier, NZ - 1 + NDP * NCHAN - 1)

    @pl.when(shares)
    def _():
        z_send(tsend, trecv, t_ss, t_rs, 0, NZ - 1)

    z_send(g1s, g1r, g_ss, g_rs, 0, NZ - 1)
    trecv[z] = tsend[z]
    g1r[z] = g1s[z]

    x8[:, 8 * J :, :] = jnp.zeros((8, CH * 2 - 8 * J, Q), BF)
    for k in range(4):
        rows = si[:, 16 * k : 16 * k + 16, :].astype(F32)
        for h in range(2):
            x8[2 * k + h, : 8 * J, :] = rows[:, 8 * h : 8 * h + 8, :].reshape(8 * J, Q).astype(BF)

    zero = jnp.zeros((ROWS, ROWS - 720), BF)
    r_syn[:, 720:] = zero

    def rows_of(ib, c):
        r = iota((128, ROWS), 0) + ib * 128
        pick = one_hot(iota((128, ROWS), 1) == (r % 4) * (NZ * LB) + r // 4)
        flat = leg[...].reshape(ROWS, 720)
        at = pl.ds(pl.multiple_of(ib * 128, 128), 128)
        r_syn[at, :720] = dot(pick, flat).astype(BF)
        return c

    lax.fori_loop(0, ROWS // 128, rows_of, 0)

    def table(src, dst):
        def step(zz, c):
            at, off = window(zz)
            r, k = iota((256, CH), 0), iota((256, CH), 1)
            pick = one_hot((r == off + k // 4) & (k < MB * J))
            full = dot(src[:, at], pick)
            keep = iota((ROWS, CH), 0) % 4 == iota((ROWS, CH), 1) % 4
            dst[zz] = jnp.where(keep, full, 0.0).astype(BF)
            return c

        lax.fori_loop(0, NZ, step, 0)

    table(r_syn, t_syn)

    def a_copy(to, frm):
        return pltpu.make_async_remote_copy(
            src_ref=trecv, dst_ref=tall.at[frm], send_sem=a_ss.at[to], recv_sem=a_rs.at[frm],
            device_id={"dp": to // NCHAN, "chan": to % NCHAN}, device_id_type=MESH,
        )

    @pl.when(shares)
    def _():
        z_wait_all(tsend, trecv, t_ss, t_rs)

        def a_send(s, c):
            a_copy((me + s + 1) % (NDP * NCHAN), me).start()
            return c

        lax.fori_loop(0, NDP * NCHAN - 1, a_send, 0)
        tall[me] = trecv[...]

    def sort_block(ib, c):
        at = pl.ds(pl.multiple_of(ib * 128, 128), 128)
        r, k = iota((128, ROWS), 0) + ib * 128, iota((128, ROWS), 1)
        p_sort[at, :] = one_hot(k == ((r % M) // 4) * 48 + (r // M) * 4 + r % 4)
        p_merge[at, :] = one_hot(k == ((r % M) // 8) * 96 + (r // M) * 8 + r % 8)
        p_unsort[at, :] = one_hot(k == ((r % 96) // 8) * M + (r // 96) * 8 + r % 8)
        return c

    lax.fori_loop(0, ROWS // 128, sort_block, 0)

    r, k = iota((128, 2 * CH), 0), iota((128, 2 * CH), 1)
    e_col[...] = one_hot((r == (k % 2) * 64 + k // 8) & (k < 8 * J))
    r, k = iota((8 * J, 128), 0), iota((8 * J, 128), 1)
    e_row[...] = one_hot(k == (r % 2) * 64 + r // 8)
    keep_f[...] = one_hot(iota((CH, 2 * CH), 0) % 8 == iota((CH, 2 * CH), 1) % 8)
    keep_b[...] = one_hot(iota((8 * J, CH), 0) % 8 == iota((8 * J, CH), 1) % 8)

    ra, ca = iota((Q, Q), 0), iota((Q, Q), 1)
    swap = jnp.where(ca == ra + 1, 1.0, 0.0) * jnp.where(ra % 2 == 0, 1.0, 0.0)
    swap = (swap - jnp.where(ra == ca + 1, 1.0, 0.0) * jnp.where(ca % 2 == 0, 1.0, 0.0)).astype(BF)
    r2, c2 = iota((256, 256), 0), iota((256, 256), 1)
    weave = one_hot(c2 == (r2 % 2) * 128 + r2 // 2)

    def weave_weight(l, c):
        for k in range(4):
            block = w[l, pl.ds(128 * k, 128), :]
            both = jnp.concatenate([block, dot(block, swap).astype(BF)], axis=0)
            w2[l, pl.ds(256 * k, 256), :] = dot(weave, both).astype(BF)
        return c

    lax.fori_loop(0, LB, weave_weight, 0)

    def legendre_sum(t, send, recv, ss, rs, out):
        acc[...] = dot(t[z], recv[z])

        def step(s, c):
            frm = z_wait_recv(send, recv, ss, rs, s)
            acc[...] += dot(t[frm], recv[frm])
            return c

        lax.fori_loop(0, NZ - 1, step, 0)
        out[...] = acc[...].astype(BF).reshape(NZ, LB * MB, Q)

    legendre_sum(t_syn, g1s, g1r, g_ss, g_rs, g2s)
    z_send(g2s, g2r, g2_ss, g2_rs, 0, NZ - 1)
    g2r[z] = g2s[z]

    def a_wait(s, c):
        @pl.when(s != me)
        def _():
            a_copy(s, s).wait_recv()

        return c

    lax.fori_loop(0, SHARES, a_wait, 0)
    rx, cx = iota((128, 64), 0), iota((128, 64), 1)
    spread = one_hot(cx == ((rx % 8) // 2) * 16 + rx // 8)

    def by_degree(lg, c):
        at = pl.ds(pl.multiple_of(lg * 128, 128), 128)
        for g in range(8):
            tiles = [tall[2 * lg + t % 2, 2 * g + t // 2] for t in range(4)]
            xr[g, at, :] = dot(spread, jnp.concatenate(tiles, axis=0)).astype(BF)
        return c

    lax.fori_loop(0, 12, by_degree, 0)

    def both_of(g, d0, d1):
        a = xr[g, pl.ds(pl.multiple_of(d0 * 96, 32), 96), :]
        b = xr[g, pl.ds(pl.multiple_of(d1 * 96, 32), 96), :]
        return jnp.concatenate([a, b], axis=0)

    def own_terms(d0, d1):
        for g in range(8):
            t_f[g] = dot(both_of(g, d0, d1), e_col[...]).astype(BF) * keep_f[...]
        for g in range(8):
            own[g] = dot(t_f[g], x8[g])

    def p_copy(side, hop, part):
        to = (z + (1 if side == 0 else NZ - 1)) % NZ
        at = pl.ds(2 * part, 2)
        return pltpu.make_async_remote_copy(
            src_ref=part_r.at[side, hop - 1, at], dst_ref=part_r.at[side, hop, at],
            send_sem=p_ss.at[side, hop - 1, part], recv_sem=p_rs.at[side, hop - 1, part],
            device_id={"lat": to}, device_id_type=MESH,
        )

    def p_send(side, hop, part, arrived):
        at = pl.ds(2 * part, 2)
        value = own[2 * part : 2 * part + 2, 96 * side : 96 * side + 96, :]
        if arrived:
            p_copy(side, hop - 1, part).wait_recv()
            value = value + part_r[side, hop - 1, at].astype(F32)
        part_r[side, hop - 1, at] = value.astype(BF)
        p_copy(side, hop, part).start()

    half_way = (z + NZ // 2) % NZ
    own_terms(half_way, half_way)
    for part in range(4):
        p_send(part // 2, 1, part, False)
    own_terms((z + 7) % NZ, (z + 9) % NZ)
    for part in range(4):
        p_send(1 - part // 2, 2, part, False)
    z_wait_all(g2s, g2r, g2_ss, g2_rs)
    grads = dot(p_sort[...], g2r[...].reshape(ROWS, Q)).astype(BF).reshape(LB, M, Q)
    gall[dp] = grads

    def mix(l, c):
        full = dot(gall[dp, l], w2[l], ((1,), (1,))).astype(BF)
        for k in range(NCHAN):
            ks[k, l] = full[:, 128 * k : 128 * k + 128]
        return c

    lax.fori_loop(0, LB, mix, 0)

    def k_copy(to, slot):
        return pltpu.make_async_remote_copy(
            src_ref=ks.at[to], dst_ref=kr.at[slot], send_sem=k_ss.at[to], recv_sem=k_rs.at[slot],
            device_id={"chan": to}, device_id_type=MESH,
        )

    def k_send(s, c):
        k_copy((ch + s + 1) % NCHAN, ch).start()
        return c

    lax.fori_loop(0, NCHAN - 1, k_send, 0)

    def d_copy(to, slot):
        return pltpu.make_async_remote_copy(
            src_ref=gall.at[dp], dst_ref=gall.at[slot], send_sem=d_ss.at[to], recv_sem=d_rs.at[slot],
            device_id={"dp": to}, device_id_type=MESH,
        )

    def d_send(s, c):
        d_copy((dp + s + 1) % NDP, dp).start()
        return c

    lax.fori_loop(0, NDP - 1, d_send, 0)
    kr[ch] = ks[ch]

    for part in range(4):
        p_send(part // 2, 2, part, True)

    def ring(hop, c):
        own_terms((z + 9 - hop) % NZ, (z + NZ - 9 + hop) % NZ)
        for part in range(4):
            for side in range(2):
                p_send(side, hop, part, True)
        return c

    lax.fori_loop(3, NZ // 2 + 1, ring, 0)

    def k_wait(s, c):
        frm = (ch + s + 1) % NCHAN
        k_copy(frm, frm).wait_recv()
        return c

    lax.fori_loop(0, NCHAN - 1, k_wait, 0)

    def sum_terms(l, c):
        total = kr[0, l].astype(F32)
        for k in range(1, NCHAN):
            total = total + kr[k, l].astype(F32)
        kr[0, l] = total.astype(BF)
        return c

    lax.fori_loop(0, LB, sum_terms, 0)
    ag[z] = dot(p_unsort[...], kr[0].reshape(ROWS, Q)).astype(BF).reshape(8, 96, Q)

    def r_copy(side, hop, part, origin):
        to = (z + (1 if side == 0 else NZ - 1)) % NZ
        at = pl.ds(2 * part, 2)
        return pltpu.make_async_remote_copy(
            src_ref=ag.at[origin, at], dst_ref=ag.at[origin, at],
            send_sem=r_ss.at[side, hop, part], recv_sem=r_rs.at[side, hop, part],
            device_id={"lat": to}, device_id_type=MESH,
        )

    for part in range(4):
        for side in range(2):
            r_copy(side, 0, part, z).start()

    home, half = ch // 2, ch % 2
    mine = sall.at[dp, half]
    own_terms(z, z)
    for part in range(4):
        at = pl.ds(2 * part, 2)
        value = own[2 * part : 2 * part + 2, :96, :]
        for side in range(2):
            p_copy(side, NZ // 2, part).wait_recv()
            value = value + part_r[side, NZ // 2, at].astype(F32)
        part_r[0, NZ // 2, at] = value.astype(BF)
    merged = part_r[0, NZ // 2].reshape(ROWS, Q)
    spectra = dot(p_merge[...], merged).astype(BF).reshape(LB, M, Q)
    s2all = ks.at[ch]
    s2all[...] = spectra

    def e_copy(to, b, h):
        return pltpu.make_async_remote_copy(
            src_ref=ks.at[ch], dst_ref=sall.at[b, h], send_sem=e_ss.at[to], recv_sem=e_rs.at[b, h],
            device_id={"dp": home, "chan": to}, device_id_type=MESH,
        )

    def e_send(s, c):
        to = (ch + s) % NCHAN

        @pl.when((to != ch) | (home != dp))
        def _():
            e_copy(to, dp, half).start()

        return c

    lax.fori_loop(0, NCHAN, e_send, 0)

    @pl.when(home == dp)
    def _():
        mine[...] = spectra

    def back_terms(d0, d1):
        for g in range(8):
            t_b[g] = dot(e_row[...], both_of(g, d0, d1), ((1,), (1,))).astype(BF) * keep_b[...]

    back_terms(z, half_way)
    for g in range(8):
        oacc[g] = dot(t_b[g, :, :96], ag[z, g])

    def hop_in(k, c):
        left, right = (z + NZ - k) % NZ, (z + k) % NZ
        back_terms(left, right)
        for part in range(4):
            for side, origin in ((0, left), (1, right)):
                r_copy(side, k - 1, part, origin).wait_recv()
                if part // 2 == side:
                    r_copy(side, k, part, origin).start()
                else:

                    @pl.when(k < NZ // 2 - 1)
                    def _():
                        r_copy(side, k, part, origin).start()

            for g in (2 * part, 2 * part + 1):
                oacc[g] += dot(t_b[g], jnp.concatenate([ag[left, g], ag[right, g]], axis=0))
        return c

    lax.fori_loop(1, NZ // 2, hop_in, 0)

    def d_wait(s, c):
        frm = (dp + s + 1) % NDP
        d_copy(frm, frm).wait_recv()
        return c

    lax.fori_loop(0, NDP - 1, d_wait, 0)
    for b in range(NDP):
        for h in range(2):

            @pl.when((b != dp) | (2 * dp + h != ch))
            def _():
                e_copy(ch, b, h).wait_recv()

    apart = one_hot(r2 == 2 * (c2 % 128) + c2 // 128)
    partner_of = (-swap.astype(F32)).astype(BF)

    def weight(l, c):
        left, right = [], []
        for b in range(NDP):
            both = jnp.concatenate([sall[b, 0, l], sall[b, 1, l]], axis=1)
            parts = dot(both, apart).astype(BF)
            left += [parts[:, :128], parts[:, 128:]]
            g = gall[b, l]
            right += [g, dot(g, partner_of).astype(BF)]
        total = dot(jnp.concatenate(left, axis=0), jnp.concatenate(right, axis=0), ((0,), (0,)))
        gw[l] = (total * 0.25).astype(BF)
        return c

    lax.fori_loop(0, LB, weight, 0)

    back_terms(half_way, half_way)
    for part in range(4):
        r_copy(part // 2, NZ // 2 - 1, part, half_way).wait_recv()
        halves = []
        for g in (2 * part, 2 * part + 1):
            halves.append((oacc[g] + dot(t_b[g, :, :96], ag[half_way, g])).reshape(J, 8, Q))
        gi[:, pl.ds(16 * part, 16), :] = jnp.concatenate(halves, axis=1).astype(BF)

    z_wait_sends(g1s, g1r, g_ss, g_rs)
    z_wait_sends(g2s, g2r, g2_ss, g2_rs)

    def p_done(hop, c):
        for part in range(4):
            for side in range(2):
                p_copy(side, hop, part).wait_send()
        return c

    lax.fori_loop(2, NZ // 2 + 1, p_done, 0)
    for part in range(4):
        p_copy(part // 2, 1, part).wait_send()

    @pl.when(shares)
    def _():
        z_wait_sends(tsend, trecv, t_ss, t_rs)

        def a_done(s, c):
            a_copy((me + s + 1) % (NDP * NCHAN), me).wait_send()
            return c

        lax.fori_loop(0, NDP * NCHAN - 1, a_done, 0)

    def r_done(k, c):
        for part in range(4):
            for side in range(2):
                r_copy(side, k, part, z).wait_send()
        return c

    lax.fori_loop(0, NZ // 2 - 1, r_done, 0)
    for part in range(4):
        r_copy(part // 2, NZ // 2 - 1, part, z).wait_send()

    def k_done(s, c):
        k_copy((ch + s + 1) % NCHAN, ch).wait_send()
        return c

    lax.fori_loop(0, NCHAN - 1, k_done, 0)

    def d_done(s, c):
        d_copy((dp + s + 1) % NDP, dp).wait_send()
        return c

    lax.fori_loop(0, NDP - 1, d_done, 0)

    def e_done(s, c):
        to = (ch + s) % NCHAN

        @pl.when((to != ch) | (home != dp))
        def _():
            e_copy(to, dp, half).wait_send()

        return c

    lax.fori_loop(0, NCHAN, e_done, 0)


def on_device(saved_input, grad_output, legendre, quad_weight, mixing_weight):
    go = grad_output[0].transpose(1, 0, 2)
    si = saved_input[0].transpose(1, 0, 2)
    vmem = pl.BlockSpec(memory_space=pltpu.VMEM)
    dma = pltpu.SemaphoreType.DMA
    gw, gi = pl.pallas_call(
        kernel,
        out_shape=(
            jax.ShapeDtypeStruct((LB, Q, Q), BF),
            jax.ShapeDtypeStruct((J, M, Q), BF),
        ),
        in_specs=[vmem] * 5,
        out_specs=(vmem, vmem),
        scratch_shapes=[
            pltpu.VMEM((ROWS, ROWS), BF), pltpu.VMEM((NZ, ROWS, CH), BF),
            pltpu.VMEM((4 * CH, 16 * J), BF),
            pltpu.VMEM((ROWS, ROWS), BF), pltpu.VMEM((ROWS, ROWS), BF), pltpu.VMEM((ROWS, ROWS), BF),
            pltpu.VMEM((LB, 1024, Q), BF),
            pltpu.VMEM((NZ, CH, Q), BF), pltpu.VMEM((NZ, CH, Q), BF),
            pltpu.VMEM((ROWS, Q), F32),
            pltpu.VMEM((NZ, LB * MB, Q), BF), pltpu.VMEM((NZ, LB * MB, Q), BF),
            pltpu.VMEM((NDP, LB, M, Q), BF), pltpu.VMEM((NDP, 2, LB, M, Q), BF),
            pltpu.VMEM((NCHAN, LB, M, Q), BF), pltpu.VMEM((NCHAN, LB, M, Q), BF),
            pltpu.VMEM((2, 16, ROWS), BF), pltpu.VMEM((NZ, 16, 128), BF), pltpu.VMEM((NZ, 16, 128), BF),
            pltpu.VMEM((SHARES, NZ, 16, 128), BF), pltpu.VMEM((8, 8 * CH, 128), BF),
            pltpu.VMEM((128, 2 * CH), BF), pltpu.VMEM((8 * J, 128), BF),
            pltpu.VMEM((CH, 2 * CH), BF), pltpu.VMEM((8 * J, CH), BF),
            pltpu.VMEM((8, 2 * CH, Q), BF), pltpu.VMEM((8, CH, 2 * CH), BF), pltpu.VMEM((8, CH, Q), F32),
            pltpu.VMEM((2, NZ // 2 + 1, 8, 96, Q), BF), pltpu.VMEM((8, 8 * J, CH), BF),
            pltpu.VMEM((NZ, 8, 96, Q), BF), pltpu.VMEM((8, 8 * J, Q), F32),
            dma((NZ,)), dma((NZ,)), dma((NZ,)), dma((NZ,)),
            dma((NCHAN,)), dma((NCHAN,)), dma((NDP,)), dma((NDP,)), dma((NCHAN,)), dma((NDP, 2)),
            dma((NZ,)), dma((NZ,)), dma((NDP * NCHAN,)), dma((SHARES,)),
            dma((2, NZ // 2, 4)), dma((2, NZ // 2, 4)), dma((2, NZ // 2, 4)), dma((2, NZ // 2, 4)),
        ],
        compiler_params=pltpu.CompilerParams(
            collective_id=0, has_side_effects=True, vmem_limit_bytes=63_000_000
        ),
    )(go, si, legendre, quad_weight, mixing_weight)
    return gw, gi.transpose(1, 0, 2)[None]


def solution(mesh):
    in_specs = (
        P("dp", None, "lat", "chan"),
        P("dp", None, "lat", "chan"),
        P("lat", None, None),
        P(),
        P("lat", None, "chan"),
    )
    out_specs = (P("lat", "dp", "chan"), P("dp", None, "lat", "chan"))
    return jax.shard_map(
        on_device, mesh=mesh, in_specs=in_specs, out_specs=out_specs, check_vma=False
    )
```

```python
import jax
import jax.numpy as jnp
from jax import lax
from jax.experimental import pallas as pl
from jax.experimental.pallas import tpu as pltpu
from jax.sharding import PartitionSpec as P

MESH = pl.DeviceIdType.MESH
BF = jnp.bfloat16
F32 = jnp.float32

M, J, Q, LB, MB, CH, NZ = 64, 45, 128, 12, 4, 192, 16
ROWS = NZ * LB * MB
NCHAN, NDP = 8, 4
SHARES = 24


def iota(shape, dim):
    return lax.broadcasted_iota(jnp.int32, shape, dim)


def dot(a, b, dims=((1,), (0,))):
    return lax.dot_general(a, b, (dims, ((), ())), preferred_element_type=F32)


def static_one(hop):
    return isinstance(hop, int) and hop == 1


def one_hot(hit):
    return jnp.where(hit, 1.0, 0.0).astype(BF)


def offset_of(s):
    k = (s + 1) // 2
    far = 8 - k
    return jnp.where(s % 2 == 1, far, NZ - far)


def kernel(
    go_in, si_in, leg_in, quad, w_in, gw, gi,
    go, si, leg, w, in_sem,
    r_syn, t_syn, p_in, p_sort, p_unsort, p_merge, w2,
    g1s, g1r, acc, g2s, g2r, gall, sall, ks, kr,
    xa, tsend, trecv, tall, xr, e_col, e_row, keep_f, keep_b, x8, t_f, own, part_r, t_b, ag, oacc, gpart,
    g_ss, g_rs, g2_ss, g2_rs, k_ss, k_rs, d_ss, d_rs, e_ss, e_rs, e1_rs, f_ss,
    t_ss, t_rs, a_ss, a_rs, p_ss, p_rs, r_ss, r_rs,
):
    dp, z, ch = lax.axis_index("dp"), lax.axis_index("lat"), lax.axis_index("chan")
    barrier = pltpu.get_barrier_semaphore()
    loads = [
        pltpu.make_async_copy(src, dst, in_sem.at[n])
        for n, (src, dst) in enumerate(((leg_in, leg), (go_in, go), (si_in, si), (w_in, w)))
    ]
    for load in loads:
        load.start()

    def greet_z(s, c):
        to = (z + s + 1) % NZ
        pl.semaphore_signal(barrier, inc=1, device_id={"lat": to}, device_id_type=MESH)
        return c

    def greet_plane(s, c):
        other = (dp * NCHAN + ch + s + 1) % (NDP * NCHAN)
        pl.semaphore_signal(
            barrier, inc=1, device_id={"dp": other // NCHAN, "chan": other % NCHAN}, device_id_type=MESH
        )
        return c

    lax.fori_loop(0, NZ - 1, greet_z, 0)
    lax.fori_loop(0, NDP * NCHAN - 1, greet_plane, 0)

    def z_copy(src, dst, ss, rs, to, slot):
        return pltpu.make_async_remote_copy(
            src_ref=src.at[to], dst_ref=dst.at[slot], send_sem=ss.at[0],
            recv_sem=rs.at[slot if rs.shape[0] > 1 else 0],
            device_id={"lat": to}, device_id_type=MESH,
        )

    def z_send(src, dst, ss, rs, first, last):
        def step(s, c):
            z_copy(src, dst, ss, rs, (z + offset_of(s)) % NZ, z).start()
            return c

        lax.fori_loop(first, last, step, 0)

    def batch(ref, count, ss, rs):
        at = ref if count is None else ref.at[pl.ds(0, count)]
        return pltpu.make_async_remote_copy(
            src_ref=at, dst_ref=at, send_sem=ss, recv_sem=rs,
            device_id={"lat": (z + 1) % NZ}, device_id_type=MESH,
        )

    for zz in range(4):
        r, c = iota((CH, 16 * J), 0), iota((CH, 16 * J), 1)
        p_in[pl.ds(zz * CH, CH), :] = one_hot((c == (r // 4) * 16 + zz * 4 + r % 4) & (r < MB * J))

    def order_in(x, out):
        def step(g, c):
            rows = x[:, pl.ds(pl.multiple_of(16 * g, 16), 16), :].reshape(16 * J, Q)
            out[pl.ds(4 * g, 4)] = dot(p_in[...], rows).astype(BF).reshape(4, CH, Q)
            return c

        lax.fori_loop(0, 4, step, 0)

    me = dp * NCHAN + ch
    shares = me < SHARES
    group, pair = jnp.minimum(me // 2, SHARES // 2 - 1), me % 2
    loads[0].wait()
    for h in range(2):
        rows = leg[2 * pair + h, pl.ds(pl.multiple_of(16 * group, 16), 16), :].astype(F32)
        xa[h, :, 720:] = jnp.zeros((16, ROWS - 720), BF)
        xa[h, :, :720] = (rows * quad[...].reshape(1, 720)).astype(BF)

    def window(zz):
        start = jnp.minimum((zz * J) // 128, 4) * 128
        return pl.ds(pl.multiple_of(start, 128), 256), zz * J - start

    def cut(i, c):
        for u in range(4):
            zz = 4 * i + u
            at, off = window(zz)
            r, k = iota((512, 128), 0), iota((512, 128), 1)
            pick = one_hot((r % 256 == off + k % 64) & (r // 256 == k // 64) & (k % 64 < J))
            both = jnp.concatenate([xa[0, :, at], xa[1, :, at]], axis=1)
            tsend[zz] = dot(both, pick).astype(BF)
        return c

    loads[1].wait()
    order_in(go, g1s)
    pl.semaphore_wait(barrier, NZ - 1 + NDP * NCHAN - 1)
    z_send(g1s, g1r, g_ss, g_rs, 0, 1)
    lax.fori_loop(0, NZ // 4, cut, 0)

    @pl.when(shares)
    def _():
        z_send(tsend, trecv, t_ss, t_rs, 0, NZ - 1)

    z_send(g1s, g1r, g_ss, g_rs, 1, NZ - 1)
    trecv[z] = tsend[z]
    g1r[z] = g1s[z]

    loads[2].wait()
    x8[:, 8 * J :, :] = jnp.zeros((8, CH * 2 - 8 * J, Q), BF)
    for k in range(4):
        rows = si[:, 16 * k : 16 * k + 16, :].astype(F32)
        for h in range(2):
            x8[2 * k + h, : 8 * J, :] = rows[:, 8 * h : 8 * h + 8, :].reshape(8 * J, Q).astype(BF)

    zero = jnp.zeros((ROWS, ROWS - 720), BF)
    r_syn[:, 720:] = zero

    def rows_of(ib, c):
        r = iota((128, ROWS), 0) + ib * 128
        pick = one_hot(iota((128, ROWS), 1) == (r % 4) * (NZ * LB) + r // 4)
        flat = leg[...].reshape(ROWS, 720)
        at = pl.ds(pl.multiple_of(ib * 128, 128), 128)
        r_syn[at, :720] = dot(pick, flat).astype(BF)
        return c

    lax.fori_loop(0, ROWS // 128, rows_of, 0)

    def table(src, dst):
        def step(zz, c):
            at, off = window(zz)
            r, k = iota((256, CH), 0), iota((256, CH), 1)
            pick = one_hot((r == off + k // 4) & (k < MB * J))
            full = dot(src[:, at], pick)
            keep = iota((ROWS, CH), 0) % 4 == iota((ROWS, CH), 1) % 4
            dst[zz] = jnp.where(keep, full, 0.0).astype(BF)
            return c

        lax.fori_loop(0, NZ, step, 0)

    table(r_syn, t_syn)

    def a_copy(to, s):
        return pltpu.make_async_remote_copy(
            src_ref=trecv, dst_ref=tall.at[me], send_sem=a_ss.at[s // SHARES], recv_sem=a_rs.at[0],
            device_id={"dp": to // NCHAN, "chan": to % NCHAN}, device_id_type=MESH,
        )

    @pl.when(shares)
    def _():
        batch(trecv, NZ - 1, t_ss.at[0], t_rs.at[0]).wait_recv()

        def a_send(s, c):
            a_copy((me + s + 1) % (NDP * NCHAN), s).start()
            return c

        lax.fori_loop(0, NDP * NCHAN - 1, a_send, 0)
        tall[me] = trecv[...]

    def sort_block(ib, c):
        at = pl.ds(pl.multiple_of(ib * 128, 128), 128)
        r, k = iota((128, ROWS), 0) + ib * 128, iota((128, ROWS), 1)
        p_sort[at, :] = one_hot(k == ((r % M) // 4) * 48 + (r // M) * 4 + r % 4)
        p_merge[at, :] = one_hot(k == ((r % M) // 8) * 96 + (r // M) * 8 + r % 8)
        p_unsort[at, :] = one_hot(k == ((r % 96) // 8) * M + (r // 96) * 8 + r % 8)
        return c

    lax.fori_loop(0, ROWS // 128, sort_block, 0)

    r, k = iota((128, 2 * CH), 0), iota((128, 2 * CH), 1)
    e_col[...] = one_hot((r == (k % 2) * 64 + k // 8) & (k < 8 * J))
    r, k = iota((8 * J, 128), 0), iota((8 * J, 128), 1)
    e_row[...] = one_hot(k == (r % 2) * 64 + r // 8)
    keep_f[...] = one_hot(iota((CH, 2 * CH), 0) % 8 == iota((CH, 2 * CH), 1) % 8)
    keep_b[...] = one_hot(iota((8 * J, CH), 0) % 8 == iota((8 * J, CH), 1) % 8)

    ra, ca = iota((Q, Q), 0), iota((Q, Q), 1)
    swap = jnp.where(ca == ra + 1, 1.0, 0.0) * jnp.where(ra % 2 == 0, 1.0, 0.0)
    swap = (swap - jnp.where(ra == ca + 1, 1.0, 0.0) * jnp.where(ca % 2 == 0, 1.0, 0.0)).astype(BF)
    r2, c2 = iota((256, 256), 0), iota((256, 256), 1)
    weave = one_hot(c2 == (r2 % 2) * 128 + r2 // 2)

    def weave_weight(l, c):
        for k in range(4):
            block = w[l, pl.ds(128 * k, 128), :]
            both = jnp.concatenate([block, dot(block, swap).astype(BF)], axis=0)
            w2[l, pl.ds(256 * k, 256), :] = dot(weave, both).astype(BF)
        return c

    loads[3].wait()
    lax.fori_loop(0, LB, weave_weight, 0)

    acc[...] = dot(t_syn[z], g1r[z])

    def latitudes(s, c):
        frm = (z + NZ - offset_of(s)) % NZ
        z_copy(g1s, g1r, g_ss, g_rs, frm, frm).wait_recv()
        acc[...] += dot(t_syn[frm], g1r[frm])
        return c

    lax.fori_loop(0, 11, latitudes, 0)

    @pl.when(shares)
    def _():
        batch(tall, SHARES - 1, a_ss.at[0], a_rs.at[0]).wait_recv()

    @pl.when(jnp.logical_not(shares))
    def _():
        batch(tall, None, a_ss.at[0], a_rs.at[0]).wait_recv()

    rx, cx = iota((128, 64), 0), iota((128, 64), 1)
    spread = one_hot(cx == ((rx % 8) // 2) * 16 + rx // 8)

    def by_degree(lg, c):
        at = pl.ds(pl.multiple_of(lg * 128, 128), 128)
        for g in range(8):
            tiles = [tall[2 * lg + t % 2, 2 * g + t // 2] for t in range(4)]
            xr[g, at, :] = dot(spread, jnp.concatenate(tiles, axis=0)).astype(BF)
        return c

    lax.fori_loop(0, 12, by_degree, 0)

    def both_of(g, d0, d1):
        a = xr[g, pl.ds(pl.multiple_of(d0 * 96, 32), 96), :]
        b = xr[g, pl.ds(pl.multiple_of(d1 * 96, 32), 96), :]
        return jnp.concatenate([a, b], axis=0)

    def own_terms(d0, d1):
        for g in range(8):
            t_f[g] = dot(both_of(g, d0, d1), e_col[...]).astype(BF) * keep_f[...]
        for g in range(8):
            own[g] = dot(t_f[g], x8[g])

    def p_copy(side, hop, part):
        to = (z + (1 if side == 0 else NZ - 1)) % NZ
        at = pl.ds(2 * part, 2)
        return pltpu.make_async_remote_copy(
            src_ref=part_r.at[side, hop - 1, at], dst_ref=part_r.at[side, hop, at],
            send_sem=p_ss.at[side, 0 if static_one(hop) else 1], recv_sem=p_rs.at[side, hop - 1, part],
            device_id={"lat": to}, device_id_type=MESH,
        )

    def p_send(side, hop, part, arrived):
        at = pl.ds(2 * part, 2)
        value = own[2 * part : 2 * part + 2, 96 * side : 96 * side + 96, :]
        if arrived:
            p_copy(side, hop - 1, part).wait_recv()
            value = value + part_r[side, hop - 1, at].astype(F32)
        part_r[side, hop - 1, at] = value.astype(BF)
        p_copy(side, hop, part).start()

    half_way = (z + NZ // 2) % NZ
    own_terms(half_way, half_way)
    for part in range(4):
        p_send(part // 2, 1, part, False)
    own_terms((z + 7) % NZ, (z + 9) % NZ)
    for part in range(4):
        p_send(1 - part // 2, 2, part, False)

    lax.fori_loop(11, NZ - 1, latitudes, 0)
    g2s[...] = acc[...].astype(BF).reshape(NZ, LB * MB, Q)
    z_send(g2s, g2r, g2_ss, g2_rs, 0, NZ - 1)
    g2r[z] = g2s[z]

    for part in range(4):
        p_send(part // 2, 2, part, True)
    own_terms((z + 6) % NZ, (z + 10) % NZ)
    batch(g2r, NZ - 1, g2_ss.at[0], g2_rs.at[0]).wait_recv()
    grads = dot(p_sort[...], g2r[...].reshape(ROWS, Q)).astype(BF).reshape(LB, M, Q)
    gall[dp] = grads

    def mix(n, c):
        for l in (3 * n, 3 * n + 1, 3 * n + 2):
            full = dot(gall[dp, l], w2[l], ((1,), (1,))).astype(BF)
            for k in range(NCHAN):
                ks[k, l] = full[:, 128 * k : 128 * k + 128]
        return c

    lax.fori_loop(0, LB // 3, mix, 0)

    def k_copy(to, slot):
        return pltpu.make_async_remote_copy(
            src_ref=ks.at[to], dst_ref=kr.at[slot], send_sem=k_ss.at[0], recv_sem=k_rs.at[0],
            device_id={"chan": to}, device_id_type=MESH,
        )

    def k_send(s, c):
        k_copy((ch + s + 1) % NCHAN, ch).start()
        return c

    lax.fori_loop(0, NCHAN - 1, k_send, 0)

    kr[ch] = ks[ch]

    def ring(hop, c):
        for part in range(4):
            for side in range(2):
                p_send(side, hop, part, True)
        own_terms((z + 8 - hop) % NZ, (z + NZ - 8 + hop) % NZ)

        @pl.when(hop == 5)
        def _():
            batch(g1s, NZ - 1, g_ss.at[0], g_rs.at[0]).wait_send()
            batch(g2s, NZ - 1, g2_ss.at[0], g2_rs.at[0]).wait_send()

        @pl.when((hop == 6) & shares)
        def _():
            batch(tsend, NZ - 1, t_ss.at[0], t_rs.at[0]).wait_send()
            batch(tall, None, a_ss.at[0], a_rs.at[0]).wait_send()
            batch(tall, NDP * NCHAN - 1 - SHARES, a_ss.at[1], a_rs.at[0]).wait_send()

        return c

    lax.fori_loop(3, NZ // 2 + 1, ring, 0)

    batch(kr, NCHAN - 1, k_ss.at[0], k_rs.at[0]).wait_recv()

    def sum_terms(l, c):
        total = kr[0, l].astype(F32)
        for k in range(1, NCHAN):
            total = total + kr[k, l].astype(F32)
        kr[0, l] = total.astype(BF)
        return c

    lax.fori_loop(0, LB, sum_terms, 0)
    ag[z] = dot(p_unsort[...], kr[0].reshape(ROWS, Q)).astype(BF).reshape(8, 96, Q)

    def r_copy(side, hop, part, origin, last=False):
        to = (z + (1 if side == 0 else NZ - 1)) % NZ
        at = pl.ds(2 * part, 2)
        return pltpu.make_async_remote_copy(
            src_ref=ag.at[origin, at], dst_ref=ag.at[origin, at],
            send_sem=r_ss.at[side, 1 if last else 0], recv_sem=r_rs.at[side, hop, part],
            device_id={"lat": to}, device_id_type=MESH,
        )

    for part in range(4):
        for side in range(2):
            r_copy(side, 0, part, z).start()

    def d_copy(to, slot):
        return pltpu.make_async_remote_copy(
            src_ref=gall.at[dp], dst_ref=gall.at[slot], send_sem=d_ss.at[0], recv_sem=d_rs.at[0],
            device_id={"dp": to}, device_id_type=MESH,
        )

    def d_send(s, c):
        d_copy((dp + s + 1) % NDP, dp).start()
        return c

    lax.fori_loop(0, NDP - 1, d_send, 0)
    home, half, row, col = ch // 2, ch % 2, ch // 4, ch % 4
    relay = (col // 2) == (dp % 2)
    own_relay = home == dp
    mine = sall.at[dp, half]
    for part in range(4):
        at = pl.ds(2 * part, 2)
        value = own[2 * part : 2 * part + 2, :96, :]
        for side in range(2):
            p_copy(side, NZ // 2, part).wait_recv()
            value = value + part_r[side, NZ // 2, at].astype(F32)
        part_r[0, NZ // 2, at] = value.astype(BF)
    merged = part_r[0, NZ // 2].reshape(ROWS, Q)
    spectra = dot(p_merge[...], merged).astype(BF)
    spectra = dot(spectra, one_hot(ra == 2 * (ca % 64) + ca // 64)).astype(BF).reshape(LB, M, Q)
    s2all = ks.at[ch]
    s2all[...] = spectra

    def e_copy(src, dst, h, to, ss, rs):
        return pltpu.make_async_remote_copy(
            src_ref=src, dst_ref=dst, send_sem=ss, recv_sem=rs,
            device_id={"dp": h, "chan": to}, device_id_type=MESH,
        )

    for h in range(2):

        @pl.when(jnp.logical_not(own_relay & (row == h)))
        def _():
            e_copy(ks.at[ch], sall.at[dp, half], home, 4 * h + col, e_ss.at[0], e1_rs.at[dp]).start()

    for h in range(2):
        to = 4 * h + (col + 2) % 4
        e_copy(ks.at[ch], sall.at[dp, half], home, to, e_ss.at[0], e_rs.at[0]).start()

    @pl.when(own_relay)
    def _():
        mine[...] = spectra

    def pass_on():
        for b in range(NDP):
            block = sall.at[b, half]

            @pl.when(jnp.logical_not(own_relay & (dp == b)))
            def _():
                e_copy(block, block, dp, ch, f_ss.at[0], e1_rs.at[b]).wait_recv()

            for side in (1, 3):
                e_copy(block, block, dp, 4 * row + (col + side) % 4, f_ss.at[0], e_rs.at[0]).start()

    def back_terms(d0, d1):
        for g in range(8):
            t_b[g] = dot(e_row[...], both_of(g, d0, d1), ((1,), (1,))).astype(BF) * keep_b[...]

    back_terms(z, half_way)
    for g in range(8):
        oacc[g] = dot(t_b[g, :, :96], ag[z, g])
    back_terms((z + NZ - 1) % NZ, (z + 1) % NZ)

    partner_of = (-swap.astype(F32)).astype(BF)

    def hop_in(k, c):
        left, right = (z + NZ - k) % NZ, (z + k) % NZ
        for part in range(4):
            for side, origin in ((0, left), (1, right)):
                r_copy(side, k - 1, part, origin).wait_recv()
                if part // 2 == side:

                    @pl.when(k < NZ // 2 - 1)
                    def _():
                        r_copy(side, k, part, origin).start()

                    @pl.when(k == NZ // 2 - 1)
                    def _():
                        r_copy(side, k, part, origin, True).start()

                else:

                    @pl.when(k < NZ // 2 - 1)
                    def _():
                        r_copy(side, k, part, origin).start()

            for g in (2 * part, 2 * part + 1):
                oacc[g] += dot(t_b[g], jnp.concatenate([ag[left, g], ag[right, g]], axis=0))
        back_terms((z + NZ - 1 - k) % NZ, (z + 1 + k) % NZ)

        @pl.when(k == 2)
        def _():
            batch(kr, NCHAN - 1, k_ss.at[0], k_rs.at[0]).wait_send()
            for side in range(2):
                batch(part_r.at[side], 7, p_ss.at[side, 1], p_rs.at[side, 0, 0]).wait_send()
                batch(part_r.at[side, 0], 4, p_ss.at[side, 0], p_rs.at[side, 0, 0]).wait_send()

        @pl.when((k == 4) & relay)
        def _():
            pass_on()

        @pl.when(k == 5)
        def _():
            batch(gall, NDP - 1, d_ss.at[0], d_rs.at[0]).wait_recv()
            for b in range(NDP):
                gpart[b] = dot(gall[b].reshape(ROWS, Q), partner_of).astype(BF).reshape(LB, M, Q)

        return c

    lax.fori_loop(1, NZ // 2, hop_in, 0)

    @pl.when(relay)
    def _():
        batch(sall, 2, e_ss.at[0], e_rs.at[0]).wait_recv()

    @pl.when(jnp.logical_not(relay))
    def _():
        batch(sall, None, e_ss.at[0], e_rs.at[0]).wait_recv()

    def weight(n, c):
        for l in (3 * n, 3 * n + 1, 3 * n + 2):
            right = jnp.concatenate(
                [jnp.concatenate([gall[b, l], gpart[b, l]], axis=1) for b in range(NDP)], axis=0
            )
            for h in range(2):
                left = jnp.concatenate([sall[b, h, l] for b in range(NDP)], axis=0)
                total = dot(left, right, ((0,), (0,)))
                gw[l, 64 * h : 64 * h + 64, :] = (
                    (total[:64, :Q] + total[64:, Q:]) * 0.25
                ).astype(BF)
        return c

    lax.fori_loop(0, LB // 3, weight, 0)

    for part in range(4):
        r_copy(part // 2, NZ // 2 - 1, part, half_way).wait_recv()
        halves = []
        for g in (2 * part, 2 * part + 1):
            halves.append((oacc[g] + dot(t_b[g, :, :96], ag[half_way, g])).reshape(J, 8, Q))
        gi[:, pl.ds(16 * part, 16), :] = jnp.concatenate(halves, axis=1).astype(BF)

    for side in range(2):
        batch(ag, 7, r_ss.at[side, 0], r_rs.at[side, 0, 0]).wait_send()
        batch(ag.at[0], 4, r_ss.at[side, 1], r_rs.at[side, 0, 0]).wait_send()
    batch(gall, NDP - 1, d_ss.at[0], d_rs.at[0]).wait_send()

    @pl.when(own_relay)
    def _():
        batch(ks, 3, e_ss.at[0], e_rs.at[0]).wait_send()

    @pl.when(jnp.logical_not(own_relay))
    def _():
        batch(ks, 4, e_ss.at[0], e_rs.at[0]).wait_send()

    @pl.when(relay)
    def _():
        batch(ks, None, f_ss.at[0], e_rs.at[0]).wait_send()


def on_device(saved_input, grad_output, legendre, quad_weight, mixing_weight):
    hbm = pl.BlockSpec(memory_space=pltpu.HBM)
    go = grad_output[0].transpose(1, 0, 2)
    si = saved_input[0].transpose(1, 0, 2)
    vmem = pl.BlockSpec(memory_space=pltpu.VMEM)
    dma = pltpu.SemaphoreType.DMA
    gw, gi = pl.pallas_call(
        kernel,
        out_shape=(
            jax.ShapeDtypeStruct((LB, Q, Q), BF),
            jax.ShapeDtypeStruct((J, M, Q), BF),
        ),
        in_specs=[hbm, hbm, hbm, vmem, hbm],
        out_specs=(vmem, vmem),
        scratch_shapes=[
            pltpu.VMEM((J, M, Q), BF), pltpu.VMEM((J, M, Q), BF),
            pltpu.VMEM((MB, CH, 720), BF), pltpu.VMEM((LB, 512, Q), BF), dma((4,)),
            pltpu.VMEM((ROWS, ROWS), BF), pltpu.VMEM((NZ, ROWS, CH), BF),
            pltpu.VMEM((4 * CH, 16 * J), BF),
            pltpu.VMEM((ROWS, ROWS), BF), pltpu.VMEM((ROWS, ROWS), BF), pltpu.VMEM((ROWS, ROWS), BF),
            pltpu.VMEM((LB, 1024, Q), BF),
            pltpu.VMEM((NZ, CH, Q), BF), pltpu.VMEM((NZ, CH, Q), BF),
            pltpu.VMEM((ROWS, Q), F32),
            pltpu.VMEM((NZ, LB * MB, Q), BF), pltpu.VMEM((NZ, LB * MB, Q), BF),
            pltpu.VMEM((NDP, LB, M, Q), BF), pltpu.VMEM((NDP, 2, LB, M, Q), BF),
            pltpu.VMEM((NCHAN, LB, M, Q), BF), pltpu.VMEM((NCHAN, LB, M, Q), BF),
            pltpu.VMEM((2, 16, ROWS), BF), pltpu.VMEM((NZ, 16, 128), BF), pltpu.VMEM((NZ, 16, 128), BF),
            pltpu.VMEM((SHARES, NZ, 16, 128), BF), pltpu.VMEM((8, 8 * CH, 128), BF),
            pltpu.VMEM((128, 2 * CH), BF), pltpu.VMEM((8 * J, 128), BF),
            pltpu.VMEM((CH, 2 * CH), BF), pltpu.VMEM((8 * J, CH), BF),
            pltpu.VMEM((8, 2 * CH, Q), BF), pltpu.VMEM((8, CH, 2 * CH), BF), pltpu.VMEM((8, CH, Q), F32),
            pltpu.VMEM((2, NZ // 2 + 1, 8, 96, Q), BF), pltpu.VMEM((8, 8 * J, CH), BF),
            pltpu.VMEM((NZ, 8, 96, Q), BF), pltpu.VMEM((8, 8 * J, Q), F32),
            pltpu.VMEM((NDP, LB, M, Q), BF),
            dma((1,)), dma((NZ,)), dma((1,)), dma((1,)), dma((1,)), dma((1,)), dma((1,)), dma((1,)),
            dma((1,)), dma((1,)), dma((NDP,)), dma((1,)), dma((1,)), dma((1,)), dma((2,)), dma((1,)),
            dma((2, 2)), dma((2, NZ // 2, 4)), dma((2, 2)), dma((2, NZ // 2, 4)),
        ],
        compiler_params=pltpu.CompilerParams(
            collective_id=0, has_side_effects=True, vmem_limit_bytes=55_000_000
        ),
    )(go, si, legendre, quad_weight, mixing_weight)
    return gw, gi.transpose(1, 0, 2)[None]


def solution(mesh):
    in_specs = (
        P("dp", None, "lat", "chan"),
        P("dp", None, "lat", "chan"),
        P("lat", None, None),
        P(),
        P("lat", None, "chan"),
    )
    out_specs = (P("lat", "dp", "chan"), P("dp", None, "lat", "chan"))
    return jax.shard_map(
        on_device, mesh=mesh, in_specs=in_specs, out_specs=out_specs, check_vma=False
    )
```

```python
import jax
import jax.numpy as jnp
from jax import lax
from jax.experimental import pallas as pl
from jax.experimental.pallas import tpu as pltpu
from jax.sharding import PartitionSpec as P

MESH = pl.DeviceIdType.MESH
BF = jnp.bfloat16
F32 = jnp.float32

M, J, Q, LB, MB, CH, NZ = 64, 45, 128, 12, 4, 192, 16
ROWS = NZ * LB * MB
NCHAN, NDP = 8, 4
GROWS = 184
SHARES = 24


def iota(shape, dim):
    return lax.broadcasted_iota(jnp.int32, shape, dim)


def dot(a, b, dims=((1,), (0,))):
    return lax.dot_general(a, b, (dims, ((), ())), preferred_element_type=F32)


def static_one(hop):
    return isinstance(hop, int) and hop == 1


def one_hot(hit):
    return jnp.where(hit, 1.0, 0.0).astype(BF)


def offset_of(s):
    k = (s + 1) // 2
    far = 8 - k
    return jnp.where(s % 2 == 1, far, NZ - far)


def kernel(
    go_in, si_in, leg_in, quad, w_in, gw, gi,
    go, si, leg, w, in_sem,
    r_syn, t_syn, p_in, p_sort, p_unsort, p_merge, w2,
    g1s, g1r, acc, g2s, g2r, gall, sall, ks, kr,
    xa, tsend, trecv, tall, xr, e_col, e_row, keep_f, keep_b, x8, t_f, own, part_r, t_b, ag, oacc, gpart,
    g_ss, g_rs, g2_ss, g2_rs, k_ss, k_rs, d_ss, d_rs, e_ss, e_rs, e1_rs, f_ss,
    t_ss, t_rs, a_ss, a_rs, p_ss, p_rs, r_ss, r_rs,
):
    dp, z, ch = lax.axis_index("dp"), lax.axis_index("lat"), lax.axis_index("chan")
    barrier = pltpu.get_barrier_semaphore()
    loads = [
        pltpu.make_async_copy(src, dst, in_sem.at[n])
        for n, (src, dst) in enumerate(((leg_in, leg), (go_in, go), (si_in, si), (w_in, w)))
    ]
    for load in loads:
        load.start()
    g1r[:, MB * J - 4 :, :] = jnp.zeros((NZ, CH - MB * J + 4, Q), BF)

    def greet_z(s, c):
        to = (z + s + 1) % NZ
        pl.semaphore_signal(barrier, inc=1, device_id={"lat": to}, device_id_type=MESH)
        return c

    def greet_plane(s, c):
        other = (dp * NCHAN + ch + s + 1) % (NDP * NCHAN)
        pl.semaphore_signal(
            barrier, inc=1, device_id={"dp": other // NCHAN, "chan": other % NCHAN}, device_id_type=MESH
        )
        return c

    lax.fori_loop(0, NZ - 1, greet_z, 0)
    lax.fori_loop(0, NDP * NCHAN - 1, greet_plane, 0)

    def z_copy(src, dst, ss, rs, to, slot):
        return pltpu.make_async_remote_copy(
            src_ref=src.at[to], dst_ref=dst.at[slot], send_sem=ss.at[0],
            recv_sem=rs.at[slot if rs.shape[0] > 1 else 0],
            device_id={"lat": to}, device_id_type=MESH,
        )

    def z_send(src, dst, ss, rs, first, last):
        def step(s, c):
            z_copy(src, dst, ss, rs, (z + offset_of(s)) % NZ, z).start()
            return c

        lax.fori_loop(first, last, step, 0)

    def g_copy(to, slot):
        at = pl.ds(0, GROWS)
        return pltpu.make_async_remote_copy(
            src_ref=g1s.at[to, at], dst_ref=g1r.at[slot, at], send_sem=g_ss.at[0],
            recv_sem=g_rs.at[slot], device_id={"lat": to}, device_id_type=MESH,
        )

    def batch(ref, count, ss, rs):
        at = ref if count is None else ref.at[pl.ds(0, count)]
        return pltpu.make_async_remote_copy(
            src_ref=at, dst_ref=at, send_sem=ss, recv_sem=rs,
            device_id={"lat": (z + 1) % NZ}, device_id_type=MESH,
        )

    for zz in range(4):
        r, c = iota((CH, 16 * J), 0), iota((CH, 16 * J), 1)
        p_in[pl.ds(zz * CH, CH), :] = one_hot((c == (r // 4) * 16 + zz * 4 + r % 4) & (r < MB * J))

    me = dp * NCHAN + ch
    shares = me < SHARES
    group, pair = jnp.minimum(me // 2, SHARES // 2 - 1), me % 2
    loads[0].wait()
    for h in range(2):
        rows = leg[2 * pair + h, pl.ds(pl.multiple_of(16 * group, 16), 16), :].astype(F32)
        xa[h, :, 720:] = jnp.zeros((16, ROWS - 720), BF)
        xa[h, :, :720] = (rows * quad[...].reshape(1, 720)).astype(BF)

    def window(zz):
        start = jnp.minimum((zz * J) // 128, 4) * 128
        return pl.ds(pl.multiple_of(start, 128), 256), zz * J - start

    def cut(i, c):
        for u in range(4):
            zz = 4 * i + u
            at, off = window(zz)
            r, k = iota((512, 128), 0), iota((512, 128), 1)
            pick = one_hot((r % 256 == off + k % 64) & (r // 256 == k // 64) & (k % 64 < J))
            both = jnp.concatenate([xa[0, :, at], xa[1, :, at]], axis=1)
            tsend[zz] = dot(both, pick).astype(BF)
        return c

    loads[1].wait()
    pl.semaphore_wait(barrier, NZ - 1 + NDP * NCHAN - 1)

    def send_group(i, c):
        g = (z // 4 + 2 + i) % 4
        rows = go[:, pl.ds(pl.multiple_of(16 * g, 16), 16), :].reshape(16 * J, Q)
        g1s[pl.ds(4 * g, 4)] = dot(p_in[...], rows).astype(BF).reshape(4, CH, Q)
        for u in range(4):
            to = 4 * g + u

            @pl.when(to != z)
            def _():
                g_copy(to, z).start()

        return c

    send_group(0, 0)
    lax.fori_loop(0, NZ // 4, cut, 0)

    @pl.when(shares)
    def _():
        z_send(tsend, trecv, t_ss, t_rs, 0, NZ - 1)

    lax.fori_loop(1, 4, send_group, 0)
    trecv[z] = tsend[z]
    g1r[z] = g1s[z]

    loads[2].wait()
    x8[:, 8 * J :, :] = jnp.zeros((8, CH * 2 - 8 * J, Q), BF)
    for k in range(4):
        rows = si[:, 16 * k : 16 * k + 16, :].astype(F32)
        for h in range(2):
            x8[2 * k + h, : 8 * J, :] = rows[:, 8 * h : 8 * h + 8, :].reshape(8 * J, Q).astype(BF)

    zero = jnp.zeros((ROWS, ROWS - 720), BF)
    r_syn[:, 720:] = zero

    def rows_of(ib, c):
        r = iota((128, ROWS), 0) + ib * 128
        pick = one_hot(iota((128, ROWS), 1) == (r % 4) * (NZ * LB) + r // 4)
        flat = leg[...].reshape(ROWS, 720)
        at = pl.ds(pl.multiple_of(ib * 128, 128), 128)
        r_syn[at, :720] = dot(pick, flat).astype(BF)
        return c

    lax.fori_loop(0, ROWS // 128, rows_of, 0)

    def table(src, dst):
        def step(zz, c):
            at, off = window(zz)
            r, k = iota((256, CH), 0), iota((256, CH), 1)
            pick = one_hot((r == off + k // 4) & (k < MB * J))
            full = dot(src[:, at], pick)
            keep = iota((ROWS, CH), 0) % 4 == iota((ROWS, CH), 1) % 4
            dst[zz] = jnp.where(keep, full, 0.0).astype(BF)
            return c

        lax.fori_loop(0, NZ, step, 0)

    table(r_syn, t_syn)

    def a_copy(to, s):
        return pltpu.make_async_remote_copy(
            src_ref=trecv, dst_ref=tall.at[me], send_sem=a_ss.at[s // SHARES], recv_sem=a_rs.at[0],
            device_id={"dp": to // NCHAN, "chan": to % NCHAN}, device_id_type=MESH,
        )

    @pl.when(shares)
    def _():
        batch(trecv, NZ - 1, t_ss.at[0], t_rs.at[0]).wait_recv()

        def a_send(s, c):
            a_copy((me + s + 1) % (NDP * NCHAN), s).start()
            return c

        lax.fori_loop(0, NDP * NCHAN - 1, a_send, 0)
        tall[me] = trecv[...]

    def sort_block(ib, c):
        at = pl.ds(pl.multiple_of(ib * 128, 128), 128)
        r, k = iota((128, ROWS), 0) + ib * 128, iota((128, ROWS), 1)
        p_sort[at, :] = one_hot(k == ((r % M) // 4) * 48 + (r // M) * 4 + r % 4)
        p_merge[at, :] = one_hot(k == ((r % M) // 8) * 96 + (r // M) * 8 + r % 8)
        p_unsort[at, :] = one_hot(k == ((r % 96) // 8) * M + (r // 96) * 8 + r % 8)
        return c

    lax.fori_loop(0, ROWS // 128, sort_block, 0)

    r, k = iota((128, 2 * CH), 0), iota((128, 2 * CH), 1)
    e_col[...] = one_hot((r == (k % 2) * 64 + k // 8) & (k < 8 * J))
    r, k = iota((8 * J, 128), 0), iota((8 * J, 128), 1)
    e_row[...] = one_hot(k == (r % 2) * 64 + r // 8)
    keep_f[...] = one_hot(iota((CH, 2 * CH), 0) % 8 == iota((CH, 2 * CH), 1) % 8)
    keep_b[...] = one_hot(iota((8 * J, CH), 0) % 8 == iota((8 * J, CH), 1) % 8)

    ra, ca = iota((Q, Q), 0), iota((Q, Q), 1)
    swap = jnp.where(ca == ra + 1, 1.0, 0.0) * jnp.where(ra % 2 == 0, 1.0, 0.0)
    swap = (swap - jnp.where(ra == ca + 1, 1.0, 0.0) * jnp.where(ca % 2 == 0, 1.0, 0.0)).astype(BF)
    r2, c2 = iota((256, 256), 0), iota((256, 256), 1)
    weave = one_hot(c2 == (r2 % 2) * 128 + r2 // 2)

    def weave_weight(l, c):
        for k in range(4):
            block = w[l, pl.ds(128 * k, 128), :]
            both = jnp.concatenate([block, dot(block, swap).astype(BF)], axis=0)
            w2[l, pl.ds(256 * k, 256), :] = dot(weave, both).astype(BF)
        return c

    loads[3].wait()
    lax.fori_loop(0, LB, weave_weight, 0)

    acc[...] = dot(t_syn[z], g1r[z])

    def latitudes(s, c):
        frm = (z + NZ - offset_of(s)) % NZ
        g_copy(frm, frm).wait_recv()
        acc[...] += dot(t_syn[frm], g1r[frm])
        return c

    lax.fori_loop(0, NZ - 1, latitudes, 0)
    g2s[...] = acc[...].astype(BF).reshape(NZ, LB * MB, Q)
    z_send(g2s, g2r, g2_ss, g2_rs, 0, NZ - 1)
    g2r[z] = g2s[z]

    @pl.when(shares)
    def _():
        batch(tall, SHARES - 1, a_ss.at[0], a_rs.at[0]).wait_recv()

    @pl.when(jnp.logical_not(shares))
    def _():
        batch(tall, None, a_ss.at[0], a_rs.at[0]).wait_recv()

    rx, cx = iota((128, 64), 0), iota((128, 64), 1)
    spread = one_hot(cx == ((rx % 8) // 2) * 16 + rx // 8)

    def by_degree(lg, c):
        at = pl.ds(pl.multiple_of(lg * 128, 128), 128)
        for g in range(8):
            tiles = [tall[2 * lg + t % 2, 2 * g + t // 2] for t in range(4)]
            xr[g, at, :] = dot(spread, jnp.concatenate(tiles, axis=0)).astype(BF)
        return c

    lax.fori_loop(0, 12, by_degree, 0)

    def both_of(g, d0, d1):
        a = xr[g, pl.ds(pl.multiple_of(d0 * 96, 32), 96), :]
        b = xr[g, pl.ds(pl.multiple_of(d1 * 96, 32), 96), :]
        return jnp.concatenate([a, b], axis=0)

    def own_terms(d0, d1):
        for g in range(8):
            t_f[g] = dot(both_of(g, d0, d1), e_col[...]).astype(BF) * keep_f[...]
        for g in range(8):
            own[g] = dot(t_f[g], x8[g])

    def p_copy(side, hop, part):
        to = (z + (1 if side == 0 else NZ - 1)) % NZ
        at = pl.ds(2 * part, 2)
        return pltpu.make_async_remote_copy(
            src_ref=part_r.at[side, hop - 1, at], dst_ref=part_r.at[side, hop, at],
            send_sem=p_ss.at[side, 0 if static_one(hop) else 1], recv_sem=p_rs.at[side, hop - 1, part],
            device_id={"lat": to}, device_id_type=MESH,
        )

    def p_send(side, hop, part, arrived):
        at = pl.ds(2 * part, 2)
        value = own[2 * part : 2 * part + 2, 96 * side : 96 * side + 96, :]
        if arrived:
            p_copy(side, hop - 1, part).wait_recv()
            value = value + part_r[side, hop - 1, at].astype(F32)
        part_r[side, hop - 1, at] = value.astype(BF)
        p_copy(side, hop, part).start()

    half_way = (z + NZ // 2) % NZ
    own_terms(half_way, half_way)
    for part in range(4):
        p_send(part // 2, 1, part, False)
    own_terms((z + 7) % NZ, (z + 9) % NZ)
    for part in range(4):
        p_send(1 - part // 2, 2, part, False)

    batch(g2r, NZ - 1, g2_ss.at[0], g2_rs.at[0]).wait_recv()
    grads = dot(p_sort[...], g2r[...].reshape(ROWS, Q)).astype(BF).reshape(LB, M, Q)
    gall[dp] = grads

    def mix(n, c):
        for l in (3 * n, 3 * n + 1, 3 * n + 2):
            full = dot(gall[dp, l], w2[l], ((1,), (1,))).astype(BF)
            for k in range(NCHAN):
                ks[k, l] = full[:, 128 * k : 128 * k + 128]
        return c

    lax.fori_loop(0, LB // 3, mix, 0)

    def k_copy(to, slot):
        return pltpu.make_async_remote_copy(
            src_ref=ks.at[to], dst_ref=kr.at[slot], send_sem=k_ss.at[0], recv_sem=k_rs.at[0],
            device_id={"chan": to}, device_id_type=MESH,
        )

    def k_send(s, c):
        k_copy((ch + s + 1) % NCHAN, ch).start()
        return c

    lax.fori_loop(0, NCHAN - 1, k_send, 0)

    kr[ch] = ks[ch]
    for part in range(4):
        p_send(part // 2, 2, part, True)
    own_terms((z + 6) % NZ, (z + 10) % NZ)

    def ring(hop, c):
        for part in range(4):
            for side in range(2):
                p_send(side, hop, part, True)
        own_terms((z + 8 - hop) % NZ, (z + NZ - 8 + hop) % NZ)

        @pl.when(hop == 5)
        def _():
            batch(g1s.at[:, pl.ds(0, GROWS)], NZ - 1, g_ss.at[0], g_rs.at[0]).wait_send()
            batch(g2s, NZ - 1, g2_ss.at[0], g2_rs.at[0]).wait_send()

        @pl.when((hop == 6) & shares)
        def _():
            batch(tsend, NZ - 1, t_ss.at[0], t_rs.at[0]).wait_send()
            batch(tall, None, a_ss.at[0], a_rs.at[0]).wait_send()
            batch(tall, NDP * NCHAN - 1 - SHARES, a_ss.at[1], a_rs.at[0]).wait_send()

        return c

    lax.fori_loop(3, NZ // 2 + 1, ring, 0)

    batch(kr, NCHAN - 1, k_ss.at[0], k_rs.at[0]).wait_recv()

    def sum_terms(l, c):
        total = kr[0, l].astype(F32)
        for k in range(1, NCHAN):
            total = total + kr[k, l].astype(F32)
        kr[0, l] = total.astype(BF)
        return c

    lax.fori_loop(0, LB, sum_terms, 0)
    ag[z] = dot(p_unsort[...], kr[0].reshape(ROWS, Q)).astype(BF).reshape(8, 96, Q)

    def r_copy(side, hop, part, origin, last=False):
        to = (z + (1 if side == 0 else NZ - 1)) % NZ
        at = pl.ds(2 * part, 2)
        return pltpu.make_async_remote_copy(
            src_ref=ag.at[origin, at], dst_ref=ag.at[origin, at],
            send_sem=r_ss.at[side, 1 if last else 0], recv_sem=r_rs.at[side, hop, part],
            device_id={"lat": to}, device_id_type=MESH,
        )

    for part in range(4):
        for side in range(2):
            r_copy(side, 0, part, z).start()

    def d_copy(to, slot):
        return pltpu.make_async_remote_copy(
            src_ref=gall.at[dp], dst_ref=gall.at[slot], send_sem=d_ss.at[0], recv_sem=d_rs.at[0],
            device_id={"dp": to}, device_id_type=MESH,
        )

    def d_send(s, c):
        d_copy((dp + s + 1) % NDP, dp).start()
        return c

    lax.fori_loop(0, NDP - 1, d_send, 0)
    home, half, row, col = ch // 2, ch % 2, ch // 4, ch % 4
    relay = (col // 2) == (dp % 2)
    own_relay = home == dp
    mine = sall.at[dp, half]
    for part in range(4):
        at = pl.ds(2 * part, 2)
        value = own[2 * part : 2 * part + 2, :96, :]
        for side in range(2):
            p_copy(side, NZ // 2, part).wait_recv()
            value = value + part_r[side, NZ // 2, at].astype(F32)
        part_r[0, NZ // 2, at] = value.astype(BF)
    merged = part_r[0, NZ // 2].reshape(ROWS, Q)
    spectra = dot(p_merge[...], merged).astype(BF)
    spectra = dot(spectra, one_hot(ra == 2 * (ca % 64) + ca // 64)).astype(BF).reshape(LB, M, Q)
    s2all = ks.at[ch]
    s2all[...] = spectra

    def e_copy(src, dst, h, to, ss, rs):
        return pltpu.make_async_remote_copy(
            src_ref=src, dst_ref=dst, send_sem=ss, recv_sem=rs,
            device_id={"dp": h, "chan": to}, device_id_type=MESH,
        )

    for h in range(2):

        @pl.when(jnp.logical_not(own_relay & (row == h)))
        def _():
            e_copy(ks.at[ch], sall.at[dp, half], home, 4 * h + col, e_ss.at[0], e1_rs.at[dp]).start()

    for h in range(2):
        to = 4 * h + (col + 2) % 4
        e_copy(ks.at[ch], sall.at[dp, half], home, to, e_ss.at[0], e_rs.at[0]).start()

    @pl.when(own_relay)
    def _():
        mine[...] = spectra

    def pass_on():
        for b in range(NDP):
            block = sall.at[b, half]

            @pl.when(jnp.logical_not(own_relay & (dp == b)))
            def _():
                e_copy(block, block, dp, ch, f_ss.at[0], e1_rs.at[b]).wait_recv()

            for side in (1, 3):
                e_copy(block, block, dp, 4 * row + (col + side) % 4, f_ss.at[0], e_rs.at[0]).start()

    def back_terms(d0, d1):
        for g in range(8):
            t_b[g] = dot(e_row[...], both_of(g, d0, d1), ((1,), (1,))).astype(BF) * keep_b[...]

    back_terms(z, half_way)
    for g in range(8):
        oacc[g] = dot(t_b[g, :, :96], ag[z, g])
    back_terms((z + NZ - 1) % NZ, (z + 1) % NZ)

    partner_of = (-swap.astype(F32)).astype(BF)

    def hop_in(k, c):
        left, right = (z + NZ - k) % NZ, (z + k) % NZ
        for part in range(4):
            for side, origin in ((0, left), (1, right)):
                r_copy(side, k - 1, part, origin).wait_recv()
                if part // 2 == side:

                    @pl.when(k < NZ // 2 - 1)
                    def _():
                        r_copy(side, k, part, origin).start()

                    @pl.when(k == NZ // 2 - 1)
                    def _():
                        r_copy(side, k, part, origin, True).start()

                else:

                    @pl.when(k < NZ // 2 - 1)
                    def _():
                        r_copy(side, k, part, origin).start()

            for g in (2 * part, 2 * part + 1):
                oacc[g] += dot(t_b[g], jnp.concatenate([ag[left, g], ag[right, g]], axis=0))
        back_terms((z + NZ - 1 - k) % NZ, (z + 1 + k) % NZ)

        @pl.when(k == 2)
        def _():
            batch(kr, NCHAN - 1, k_ss.at[0], k_rs.at[0]).wait_send()
            for side in range(2):
                batch(part_r.at[side], 7, p_ss.at[side, 1], p_rs.at[side, 0, 0]).wait_send()
                batch(part_r.at[side, 0], 4, p_ss.at[side, 0], p_rs.at[side, 0, 0]).wait_send()

        @pl.when((k == 4) & relay)
        def _():
            pass_on()

        @pl.when(k == 5)
        def _():
            batch(gall, NDP - 1, d_ss.at[0], d_rs.at[0]).wait_recv()
            for b in range(NDP):
                gpart[b] = dot(gall[b].reshape(ROWS, Q), partner_of).astype(BF).reshape(LB, M, Q)

        return c

    lax.fori_loop(1, NZ // 2, hop_in, 0)

    @pl.when(relay)
    def _():
        batch(sall, 2, e_ss.at[0], e_rs.at[0]).wait_recv()

    @pl.when(jnp.logical_not(relay))
    def _():
        batch(sall, None, e_ss.at[0], e_rs.at[0]).wait_recv()

    def weight(n, c):
        for l in (3 * n, 3 * n + 1, 3 * n + 2):
            right = jnp.concatenate(
                [jnp.concatenate([gall[b, l], gpart[b, l]], axis=1) for b in range(NDP)], axis=0
            )
            for h in range(2):
                left = jnp.concatenate([sall[b, h, l] for b in range(NDP)], axis=0)
                total = dot(left, right, ((0,), (0,)))
                gw[l, 64 * h : 64 * h + 64, :] = (
                    (total[:64, :Q] + total[64:, Q:]) * 0.25
                ).astype(BF)
        return c

    lax.fori_loop(0, LB // 3, weight, 0)

    for part in range(4):
        r_copy(part // 2, NZ // 2 - 1, part, half_way).wait_recv()
        halves = []
        for g in (2 * part, 2 * part + 1):
            halves.append((oacc[g] + dot(t_b[g, :, :96], ag[half_way, g])).reshape(J, 8, Q))
        gi[:, pl.ds(16 * part, 16), :] = jnp.concatenate(halves, axis=1).astype(BF)

    for side in range(2):
        batch(ag, 7, r_ss.at[side, 0], r_rs.at[side, 0, 0]).wait_send()
        batch(ag.at[0], 4, r_ss.at[side, 1], r_rs.at[side, 0, 0]).wait_send()
    batch(gall, NDP - 1, d_ss.at[0], d_rs.at[0]).wait_send()

    @pl.when(own_relay)
    def _():
        batch(ks, 3, e_ss.at[0], e_rs.at[0]).wait_send()

    @pl.when(jnp.logical_not(own_relay))
    def _():
        batch(ks, 4, e_ss.at[0], e_rs.at[0]).wait_send()

    @pl.when(relay)
    def _():
        batch(ks, None, f_ss.at[0], e_rs.at[0]).wait_send()


def on_device(saved_input, grad_output, legendre, quad_weight, mixing_weight):
    hbm = pl.BlockSpec(memory_space=pltpu.HBM)
    go = grad_output[0].transpose(1, 0, 2)
    si = saved_input[0].transpose(1, 0, 2)
    vmem = pl.BlockSpec(memory_space=pltpu.VMEM)
    dma = pltpu.SemaphoreType.DMA
    gw, gi = pl.pallas_call(
        kernel,
        out_shape=(
            jax.ShapeDtypeStruct((LB, Q, Q), BF),
            jax.ShapeDtypeStruct((J, M, Q), BF),
        ),
        in_specs=[hbm, hbm, hbm, vmem, hbm],
        out_specs=(vmem, vmem),
        scratch_shapes=[
            pltpu.VMEM((J, M, Q), BF), pltpu.VMEM((J, M, Q), BF),
            pltpu.VMEM((MB, CH, 720), BF), pltpu.VMEM((LB, 512, Q), BF), dma((4,)),
            pltpu.VMEM((ROWS, ROWS), BF), pltpu.VMEM((NZ, ROWS, CH), BF),
            pltpu.VMEM((4 * CH, 16 * J), BF),
            pltpu.VMEM((ROWS, ROWS), BF), pltpu.VMEM((ROWS, ROWS), BF), pltpu.VMEM((ROWS, ROWS), BF),
            pltpu.VMEM((LB, 1024, Q), BF),
            pltpu.VMEM((NZ, CH, Q), BF), pltpu.VMEM((NZ, CH, Q), BF),
            pltpu.VMEM((ROWS, Q), F32),
            pltpu.VMEM((NZ, LB * MB, Q), BF), pltpu.VMEM((NZ, LB * MB, Q), BF),
            pltpu.VMEM((NDP, LB, M, Q), BF), pltpu.VMEM((NDP, 2, LB, M, Q), BF),
            pltpu.VMEM((NCHAN, LB, M, Q), BF), pltpu.VMEM((NCHAN, LB, M, Q), BF),
            pltpu.VMEM((2, 16, ROWS), BF), pltpu.VMEM((NZ, 16, 128), BF), pltpu.VMEM((NZ, 16, 128), BF),
            pltpu.VMEM((SHARES, NZ, 16, 128), BF), pltpu.VMEM((8, 8 * CH, 128), BF),
            pltpu.VMEM((128, 2 * CH), BF), pltpu.VMEM((8 * J, 128), BF),
            pltpu.VMEM((CH, 2 * CH), BF), pltpu.VMEM((8 * J, CH), BF),
            pltpu.VMEM((8, 2 * CH, Q), BF), pltpu.VMEM((8, CH, 2 * CH), BF), pltpu.VMEM((8, CH, Q), F32),
            pltpu.VMEM((2, NZ // 2 + 1, 8, 96, Q), BF), pltpu.VMEM((8, 8 * J, CH), BF),
            pltpu.VMEM((NZ, 8, 96, Q), BF), pltpu.VMEM((8, 8 * J, Q), F32),
            pltpu.VMEM((NDP, LB, M, Q), BF),
            dma((1,)), dma((NZ,)), dma((1,)), dma((1,)), dma((1,)), dma((1,)), dma((1,)), dma((1,)),
            dma((1,)), dma((1,)), dma((NDP,)), dma((1,)), dma((1,)), dma((1,)), dma((2,)), dma((1,)),
            dma((2, 2)), dma((2, NZ // 2, 4)), dma((2, 2)), dma((2, NZ // 2, 4)),
        ],
        compiler_params=pltpu.CompilerParams(
            collective_id=0, has_side_effects=True, vmem_limit_bytes=55_000_000
        ),
    )(go, si, legendre, quad_weight, mixing_weight)
    return gw, gi.transpose(1, 0, 2)[None]


def solution(mesh):
    in_specs = (
        P("dp", None, "lat", "chan"),
        P("dp", None, "lat", "chan"),
        P("lat", None, None),
        P(),
        P("lat", None, "chan"),
    )
    out_specs = (P("lat", "dp", "chan"), P("dp", None, "lat", "chan"))
    return jax.shard_map(
        on_device, mesh=mesh, in_specs=in_specs, out_specs=out_specs, check_vma=False
    )
```

```python
import jax
import jax.numpy as jnp
from jax import lax
from jax.experimental import pallas as pl
from jax.experimental.pallas import tpu as pltpu
from jax.sharding import PartitionSpec as P

MESH = pl.DeviceIdType.MESH
BF = jnp.bfloat16
F32 = jnp.float32

M, J, Q, LB, MB, CH, NZ = 64, 45, 128, 12, 4, 192, 16
ROWS = NZ * LB * MB
NCHAN, NDP = 8, 4
GROWS = 184
SHARES = 24


def iota(shape, dim):
    return lax.broadcasted_iota(jnp.int32, shape, dim)


def dot(a, b, dims=((1,), (0,))):
    return lax.dot_general(a, b, (dims, ((), ())), preferred_element_type=F32)


def static_one(hop):
    return isinstance(hop, int) and hop == 1


def one_hot(hit):
    return jnp.where(hit, 1.0, 0.0).astype(BF)


def offset_of(s):
    k = (s + 1) // 2
    far = 8 - k
    return jnp.where(s % 2 == 1, far, NZ - far)


def kernel(
    go_in, si_in, leg_in, quad, w_in, gw, gi,
    go, si, leg, w, in_sem,
    r_syn, t_syn, p_in, p_sort, p_unsort, p_merge, w2,
    g1s, g1r, acc, g2s, g2r, gall, sall, ks, kr,
    xa, tsend, trecv, tall, xr, e_col, e_row, keep_f, keep_b, x8, t_f, own, part_r, t_b, ag, oacc, gpart,
    g_ss, g_rs, g2_ss, g2_rs, k_ss, k_rs, d_ss, d_rs, e_ss, e_rs, e1_rs, f_ss,
    t_ss, t_rs, a_ss, a_rs, b_ss, b_rs, p_ss, p_rs, r_ss, r_rs,
):
    dp, z, ch = lax.axis_index("dp"), lax.axis_index("lat"), lax.axis_index("chan")
    barrier = pltpu.get_barrier_semaphore()
    loads = [
        pltpu.make_async_copy(src, dst, in_sem.at[n])
        for n, (src, dst) in enumerate(((leg_in, leg), (go_in, go), (si_in, si), (w_in, w)))
    ]
    for load in loads:
        load.start()
    g1r[:, MB * J - 4 :, :] = jnp.zeros((NZ, CH - MB * J + 4, Q), BF)

    def greet_z(s, c):
        to = (z + s + 1) % NZ
        pl.semaphore_signal(barrier, inc=1, device_id={"lat": to}, device_id_type=MESH)
        return c

    def greet_plane(s, c):
        other = (dp * NCHAN + ch + s + 1) % (NDP * NCHAN)
        pl.semaphore_signal(
            barrier, inc=1, device_id={"dp": other // NCHAN, "chan": other % NCHAN}, device_id_type=MESH
        )
        return c

    lax.fori_loop(0, NZ - 1, greet_z, 0)
    lax.fori_loop(0, NDP * NCHAN - 1, greet_plane, 0)

    def z_copy(src, dst, ss, rs, to, slot):
        return pltpu.make_async_remote_copy(
            src_ref=src.at[to], dst_ref=dst.at[slot], send_sem=ss.at[0],
            recv_sem=rs.at[slot if rs.shape[0] > 1 else 0],
            device_id={"lat": to}, device_id_type=MESH,
        )

    def z_send(src, dst, ss, rs, first, last):
        def step(s, c):
            z_copy(src, dst, ss, rs, (z + offset_of(s)) % NZ, z).start()
            return c

        lax.fori_loop(first, last, step, 0)

    def g_copy(to, slot):
        at = pl.ds(0, GROWS)
        return pltpu.make_async_remote_copy(
            src_ref=g1s.at[to, at], dst_ref=g1r.at[slot, at], send_sem=g_ss.at[0],
            recv_sem=g_rs.at[slot], device_id={"lat": to}, device_id_type=MESH,
        )

    def batch(ref, count, ss, rs):
        at = ref if count is None else ref.at[pl.ds(0, count)]
        return pltpu.make_async_remote_copy(
            src_ref=at, dst_ref=at, send_sem=ss, recv_sem=rs,
            device_id={"lat": (z + 1) % NZ}, device_id_type=MESH,
        )

    for zz in range(4):
        r, c = iota((CH, 16 * J), 0), iota((CH, 16 * J), 1)
        p_in[pl.ds(zz * CH, CH), :] = one_hot((c == (r // 4) * 16 + zz * 4 + r % 4) & (r < MB * J))

    me = dp * NCHAN + ch
    shares = me < SHARES
    group, pair = jnp.minimum(me // 2, SHARES // 2 - 1), me % 2
    loads[0].wait()
    for h in range(2):
        rows = leg[2 * pair + h, pl.ds(pl.multiple_of(16 * group, 16), 16), :].astype(F32)
        xa[h, :, 720:] = jnp.zeros((16, ROWS - 720), BF)
        xa[h, :, :720] = (rows * quad[...].reshape(1, 720)).astype(BF)

    def window(zz):
        start = jnp.minimum((zz * J) // 128, 4) * 128
        return pl.ds(pl.multiple_of(start, 128), 256), zz * J - start

    def cut(i, c):
        for u in range(4):
            zz = 4 * i + u
            at, off = window(zz)
            r, k = iota((512, 128), 0), iota((512, 128), 1)
            pick = one_hot((r % 256 == off + k % 64) & (r // 256 == k // 64) & (k % 64 < J))
            both = jnp.concatenate([xa[0, :, at], xa[1, :, at]], axis=1)
            tsend[zz] = dot(both, pick).astype(BF)
        return c

    lax.fori_loop(0, NZ // 4, cut, 0)
    loads[1].wait()
    pl.semaphore_wait(barrier, NZ - 1 + NDP * NCHAN - 1)

    def send_group(i, c):
        g = (z // 4 + 2 + i) % 4
        rows = go[:, pl.ds(pl.multiple_of(16 * g, 16), 16), :].reshape(16 * J, Q)
        g1s[pl.ds(4 * g, 4)] = dot(p_in[...], rows).astype(BF).reshape(4, CH, Q)
        for u in range(4):
            to = 4 * g + u

            @pl.when(to != z)
            def _():
                g_copy(to, z).start()

        return c

    @pl.when(shares)
    def _():
        z_send(tsend, trecv, t_ss, t_rs, 0, NZ - 1)

    lax.fori_loop(0, 4, send_group, 0)
    trecv[z] = tsend[z]
    g1r[z] = g1s[z]

    loads[2].wait()
    x8[:, 8 * J :, :] = jnp.zeros((8, CH * 2 - 8 * J, Q), BF)
    for k in range(4):
        rows = si[:, 16 * k : 16 * k + 16, :].astype(F32)
        for h in range(2):
            x8[2 * k + h, : 8 * J, :] = rows[:, 8 * h : 8 * h + 8, :].reshape(8 * J, Q).astype(BF)

    zero = jnp.zeros((ROWS, ROWS - 720), BF)
    r_syn[:, 720:] = zero

    def rows_of(ib, c):
        r = iota((128, ROWS), 0) + ib * 128
        pick = one_hot(iota((128, ROWS), 1) == (r % 4) * (NZ * LB) + r // 4)
        flat = leg[...].reshape(ROWS, 720)
        at = pl.ds(pl.multiple_of(ib * 128, 128), 128)
        r_syn[at, :720] = dot(pick, flat).astype(BF)
        return c

    lax.fori_loop(0, ROWS // 128, rows_of, 0)

    def table(src, dst):
        def step(zz, c):
            at, off = window(zz)
            r, k = iota((256, CH), 0), iota((256, CH), 1)
            pick = one_hot((r == off + k // 4) & (k < MB * J))
            full = dot(src[:, at], pick)
            keep = iota((ROWS, CH), 0) % 4 == iota((ROWS, CH), 1) % 4
            dst[zz] = jnp.where(keep, full, 0.0).astype(BF)
            return c

        lax.fori_loop(0, NZ, step, 0)

    table(r_syn, t_syn)

    def sort_block(ib, c):
        at = pl.ds(pl.multiple_of(ib * 128, 128), 128)
        r, k = iota((128, ROWS), 0) + ib * 128, iota((128, ROWS), 1)
        p_sort[at, :] = one_hot(k == ((r % M) // 4) * 48 + (r // M) * 4 + r % 4)
        p_merge[at, :] = one_hot(k == ((r % M) // 8) * 96 + (r // M) * 8 + r % 8)
        p_unsort[at, :] = one_hot(k == ((r % 96) // 8) * M + (r // 96) * 8 + r % 8)
        return c

    lax.fori_loop(0, ROWS // 128, sort_block, 0)

    r, k = iota((128, 2 * CH), 0), iota((128, 2 * CH), 1)
    e_col[...] = one_hot((r == (k % 2) * 64 + k // 8) & (k < 8 * J))
    r, k = iota((8 * J, 128), 0), iota((8 * J, 128), 1)
    e_row[...] = one_hot(k == (r % 2) * 64 + r // 8)
    keep_f[...] = one_hot(iota((CH, 2 * CH), 0) % 8 == iota((CH, 2 * CH), 1) % 8)
    keep_b[...] = one_hot(iota((8 * J, CH), 0) % 8 == iota((8 * J, CH), 1) % 8)

    ra, ca = iota((Q, Q), 0), iota((Q, Q), 1)
    swap = jnp.where(ca == ra + 1, 1.0, 0.0) * jnp.where(ra % 2 == 0, 1.0, 0.0)
    swap = (swap - jnp.where(ra == ca + 1, 1.0, 0.0) * jnp.where(ca % 2 == 0, 1.0, 0.0)).astype(BF)
    r2, c2 = iota((256, 256), 0), iota((256, 256), 1)
    weave = one_hot(c2 == (r2 % 2) * 128 + r2 // 2)

    def weave_weight(l, c):
        for k in range(4):
            block = w[l, pl.ds(128 * k, 128), :]
            both = jnp.concatenate([block, dot(block, swap).astype(BF)], axis=0)
            w2[l, pl.ds(256 * k, 256), :] = dot(weave, both).astype(BF)
        return c

    loads[3].wait()
    lax.fori_loop(0, LB // 2, weave_weight, 0)

    core = dp % 2
    sibling = dp + 1 - 2 * core

    @pl.when(shares)
    def _():
        batch(trecv, NZ - 1, t_ss.at[0], t_rs.at[0]).wait_recv()

        def a_send(s, c):
            to = ((dp // 2) * NCHAN + ch + s + 1) % (2 * NCHAN)
            pltpu.make_async_remote_copy(
                src_ref=trecv, dst_ref=tall.at[me], send_sem=a_ss.at[0], recv_sem=a_rs.at[0],
                device_id={"dp": (to // NCHAN) * 2 + core, "chan": to % NCHAN}, device_id_type=MESH,
            ).start()
            return c

        lax.fori_loop(0, 2 * NCHAN - 1, a_send, 0)
        tall[me] = trecv[...]

    lax.fori_loop(LB // 2, LB, weave_weight, 0)

    def b_copy(first):
        at = tall.at[pl.ds(first, 8)]
        return pltpu.make_async_remote_copy(
            src_ref=at, dst_ref=at, send_sem=b_ss.at[0], recv_sem=b_rs.at[0],
            device_id={"dp": sibling}, device_id_type=MESH,
        )

    def to_sibling():
        @pl.when(core == 0)
        def _():
            batch(tall, 15, a_ss.at[0], a_rs.at[0]).wait_recv()
            b_copy(0).start()
            b_copy(16).start()

        @pl.when(dp == 1)
        def _():
            batch(tall, 7, a_ss.at[0], a_rs.at[0]).wait_recv()

        @pl.when(dp == 3)
        def _():
            batch(tall, 8, a_ss.at[0], a_rs.at[0]).wait_recv()

        @pl.when(core == 1)
        def _():
            b_copy(8).start()

    acc[...] = dot(t_syn[z], g1r[z])

    def latitudes(s, c):
        frm = (z + NZ - offset_of(s)) % NZ
        g_copy(frm, frm).wait_recv()
        acc[...] += dot(t_syn[frm], g1r[frm])
        return c

    lax.fori_loop(0, 6, latitudes, 0)
    to_sibling()
    lax.fori_loop(6, NZ - 1, latitudes, 0)
    g2s[...] = acc[...].astype(BF).reshape(NZ, LB * MB, Q)
    z_send(g2s, g2r, g2_ss, g2_rs, 0, NZ - 1)
    g2r[z] = g2s[z]

    @pl.when(core == 0)
    def _():
        batch(tall, 8, b_ss.at[0], b_rs.at[0]).wait_recv()

    @pl.when(core == 1)
    def _():
        batch(tall, 16, b_ss.at[0], b_rs.at[0]).wait_recv()

    rx, cx = iota((128, 64), 0), iota((128, 64), 1)
    spread = one_hot(cx == ((rx % 8) // 2) * 16 + rx // 8)

    def by_degree(lg, c):
        at = pl.ds(pl.multiple_of(lg * 128, 128), 128)
        for g in range(8):
            tiles = [tall[2 * lg + t % 2, 2 * g + t // 2] for t in range(4)]
            xr[g, at, :] = dot(spread, jnp.concatenate(tiles, axis=0)).astype(BF)
        return c

    lax.fori_loop(0, 12, by_degree, 0)

    def both_of(g, d0, d1):
        a = xr[g, pl.ds(pl.multiple_of(d0 * 96, 32), 96), :]
        b = xr[g, pl.ds(pl.multiple_of(d1 * 96, 32), 96), :]
        return jnp.concatenate([a, b], axis=0)

    def own_terms(d0, d1):
        for g in range(8):
            t_f[g] = dot(both_of(g, d0, d1), e_col[...]).astype(BF) * keep_f[...]
        for g in range(8):
            own[g] = dot(t_f[g], x8[g])

    def p_copy(side, hop, part):
        to = (z + (1 if side == 0 else NZ - 1)) % NZ
        at = pl.ds(2 * part, 2)
        return pltpu.make_async_remote_copy(
            src_ref=part_r.at[side, hop - 1, at], dst_ref=part_r.at[side, hop, at],
            send_sem=p_ss.at[side, 0 if static_one(hop) else 1], recv_sem=p_rs.at[side, hop - 1, part],
            device_id={"lat": to}, device_id_type=MESH,
        )

    def p_send(side, hop, part, arrived):
        at = pl.ds(2 * part, 2)
        value = own[2 * part : 2 * part + 2, 96 * side : 96 * side + 96, :]
        if arrived:
            p_copy(side, hop - 1, part).wait_recv()
            value = value + part_r[side, hop - 1, at].astype(F32)
        part_r[side, hop - 1, at] = value.astype(BF)
        p_copy(side, hop, part).start()

    half_way = (z + NZ // 2) % NZ
    own_terms(half_way, half_way)
    for part in range(4):
        p_send(part // 2, 1, part, False)
    own_terms((z + 7) % NZ, (z + 9) % NZ)
    for part in range(4):
        p_send(1 - part // 2, 2, part, False)

    batch(g2r, NZ - 1, g2_ss.at[0], g2_rs.at[0]).wait_recv()
    grads = dot(p_sort[...], g2r[...].reshape(ROWS, Q)).astype(BF).reshape(LB, M, Q)
    gall[dp] = grads

    def mix(n, c):
        for l in (3 * n, 3 * n + 1, 3 * n + 2):
            full = dot(gall[dp, l], w2[l], ((1,), (1,))).astype(BF)
            for k in range(NCHAN):
                ks[k, l] = full[:, 128 * k : 128 * k + 128]
        return c

    lax.fori_loop(0, LB // 3, mix, 0)

    def k_copy(to, slot):
        return pltpu.make_async_remote_copy(
            src_ref=ks.at[to], dst_ref=kr.at[slot], send_sem=k_ss.at[0], recv_sem=k_rs.at[0],
            device_id={"chan": to}, device_id_type=MESH,
        )

    row, col = ch // 4, ch % 4
    for u in range(4):
        k_copy((1 - row) * 4 + (col + u) % 4, ch).start()
    for u in range(1, 4):
        k_copy(row * 4 + (col + u) % 4, ch).start()

    kr[ch] = ks[ch]
    for part in range(4):
        p_send(part // 2, 2, part, True)
    own_terms((z + 6) % NZ, (z + 10) % NZ)

    def ring(hop, c):
        for part in range(4):
            for side in range(2):
                p_send(side, hop, part, True)
        own_terms((z + 8 - hop) % NZ, (z + NZ - 8 + hop) % NZ)

        @pl.when(hop == 5)
        def _():
            batch(g1s.at[:, pl.ds(0, GROWS)], NZ - 1, g_ss.at[0], g_rs.at[0]).wait_send()
            batch(g2s, NZ - 1, g2_ss.at[0], g2_rs.at[0]).wait_send()

        @pl.when((hop == 6) & shares)
        def _():
            batch(tsend, NZ - 1, t_ss.at[0], t_rs.at[0]).wait_send()
            batch(tall, 15, a_ss.at[0], a_rs.at[0]).wait_send()

        @pl.when((hop == 6) & (core == 0))
        def _():
            batch(tall, 16, b_ss.at[0], b_rs.at[0]).wait_send()

        @pl.when((hop == 6) & (core == 1))
        def _():
            batch(tall, 8, b_ss.at[0], b_rs.at[0]).wait_send()

        return c

    lax.fori_loop(3, NZ // 2 + 1, ring, 0)

    batch(kr, NCHAN - 1, k_ss.at[0], k_rs.at[0]).wait_recv()

    def sum_terms(l, c):
        total = kr[0, l].astype(F32)
        for k in range(1, NCHAN):
            total = total + kr[k, l].astype(F32)
        kr[0, l] = total.astype(BF)
        return c

    lax.fori_loop(0, LB, sum_terms, 0)
    ag[z] = dot(p_unsort[...], kr[0].reshape(ROWS, Q)).astype(BF).reshape(8, 96, Q)

    def r_copy(side, hop, part, origin, last=False):
        to = (z + (1 if side == 0 else NZ - 1)) % NZ
        at = pl.ds(2 * part, 2)
        return pltpu.make_async_remote_copy(
            src_ref=ag.at[origin, at], dst_ref=ag.at[origin, at],
            send_sem=r_ss.at[side, 1 if last else 0], recv_sem=r_rs.at[side, hop, part],
            device_id={"lat": to}, device_id_type=MESH,
        )

    for part in range(4):
        for side in range(2):
            r_copy(side, 0, part, z).start()

    home, half = ch // 2, ch % 2
    relay = (col // 2) == (dp % 2)
    own_relay = home == dp
    mine = sall.at[dp, half]
    for part in range(4):
        at = pl.ds(2 * part, 2)
        value = own[2 * part : 2 * part + 2, :96, :]
        for side in range(2):
            p_copy(side, NZ // 2, part).wait_recv()
            value = value + part_r[side, NZ // 2, at].astype(F32)
        part_r[0, NZ // 2, at] = value.astype(BF)
    merged = part_r[0, NZ // 2].reshape(ROWS, Q)
    spectra = dot(p_merge[...], merged).astype(BF)
    spectra = dot(spectra, one_hot(ra == 2 * (ca % 64) + ca // 64)).astype(BF).reshape(LB, M, Q)
    s2all = ks.at[ch]
    s2all[...] = spectra

    def e_copy(src, dst, h, to, ss, rs):
        return pltpu.make_async_remote_copy(
            src_ref=src, dst_ref=dst, send_sem=ss, recv_sem=rs,
            device_id={"dp": h, "chan": to}, device_id_type=MESH,
        )

    for h in range(2):

        @pl.when(jnp.logical_not(own_relay & (row == h)))
        def _():
            e_copy(ks.at[ch], sall.at[dp, half], home, 4 * h + col, e_ss.at[0], e1_rs.at[dp]).start()

    def send_across():
        for h in range(2):
            to = 4 * h + (col + 2) % 4
            e_copy(ks.at[ch], sall.at[dp, half], home, to, e_ss.at[0], e_rs.at[0]).start()

    def d_copy(to, slot):
        return pltpu.make_async_remote_copy(
            src_ref=gall.at[dp], dst_ref=gall.at[slot], send_sem=d_ss.at[0], recv_sem=d_rs.at[0],
            device_id={"dp": to}, device_id_type=MESH,
        )

    def d_send(s, c):
        d_copy((dp + s + 1) % NDP, dp).start()
        return c

    @pl.when(own_relay)
    def _():
        mine[...] = spectra

    def pass_on():
        for b in range(NDP):
            block = sall.at[b, half]

            @pl.when(jnp.logical_not(own_relay & (dp == b)))
            def _():
                e_copy(block, block, dp, ch, f_ss.at[0], e1_rs.at[b]).wait_recv()

            for side in (1, 3):
                e_copy(block, block, dp, 4 * row + (col + side) % 4, f_ss.at[0], e_rs.at[0]).start()

    def back_terms(d0, d1):
        for g in range(8):
            t_b[g] = dot(e_row[...], both_of(g, d0, d1), ((1,), (1,))).astype(BF) * keep_b[...]

    back_terms(z, half_way)
    for g in range(8):
        oacc[g] = dot(t_b[g, :, :96], ag[z, g])
    back_terms((z + NZ - 1) % NZ, (z + 1) % NZ)

    partner_of = (-swap.astype(F32)).astype(BF)

    def hop_in(k, c):
        left, right = (z + NZ - k) % NZ, (z + k) % NZ
        for part in range(4):
            for side, origin in ((0, left), (1, right)):
                r_copy(side, k - 1, part, origin).wait_recv()
                if part // 2 == side:

                    @pl.when(k < NZ // 2 - 1)
                    def _():
                        r_copy(side, k, part, origin).start()

                    @pl.when(k == NZ // 2 - 1)
                    def _():
                        r_copy(side, k, part, origin, True).start()

                else:

                    @pl.when(k < NZ // 2 - 1)
                    def _():
                        r_copy(side, k, part, origin).start()

            for g in (2 * part, 2 * part + 1):
                oacc[g] += dot(t_b[g], jnp.concatenate([ag[left, g], ag[right, g]], axis=0))
        back_terms((z + NZ - 1 - k) % NZ, (z + 1 + k) % NZ)

        @pl.when(k == 2)
        def _():
            send_across()
            batch(kr, NCHAN - 1, k_ss.at[0], k_rs.at[0]).wait_send()
            for side in range(2):
                batch(part_r.at[side], 7, p_ss.at[side, 1], p_rs.at[side, 0, 0]).wait_send()
                batch(part_r.at[side, 0], 4, p_ss.at[side, 0], p_rs.at[side, 0, 0]).wait_send()

        @pl.when((k == 4) & relay)
        def _():
            pass_on()

        @pl.when(k == 4)
        def _():
            lax.fori_loop(0, NDP - 1, d_send, 0)

        @pl.when(k == 7)
        def _():
            batch(gall, NDP - 1, d_ss.at[0], d_rs.at[0]).wait_recv()
            for b in range(NDP):
                gpart[b] = dot(gall[b].reshape(ROWS, Q), partner_of).astype(BF).reshape(LB, M, Q)

        return c

    lax.fori_loop(1, NZ // 2, hop_in, 0)

    @pl.when(relay)
    def _():
        batch(sall, 2, e_ss.at[0], e_rs.at[0]).wait_recv()

    @pl.when(jnp.logical_not(relay))
    def _():
        batch(sall, None, e_ss.at[0], e_rs.at[0]).wait_recv()

    def weight(n, c):
        for l in (3 * n, 3 * n + 1, 3 * n + 2):
            right = jnp.concatenate(
                [jnp.concatenate([gall[b, l], gpart[b, l]], axis=1) for b in range(NDP)], axis=0
            )
            for h in range(2):
                left = jnp.concatenate([sall[b, h, l] for b in range(NDP)], axis=0)
                total = dot(left, right, ((0,), (0,)))
                gw[l, 64 * h : 64 * h + 64, :] = (
                    (total[:64, :Q] + total[64:, Q:]) * 0.25
                ).astype(BF)
        return c

    lax.fori_loop(0, LB // 3, weight, 0)

    for part in range(4):
        r_copy(part // 2, NZ // 2 - 1, part, half_way).wait_recv()
        halves = []
        for g in (2 * part, 2 * part + 1):
            halves.append((oacc[g] + dot(t_b[g, :, :96], ag[half_way, g])).reshape(J, 8, Q))
        gi[:, pl.ds(16 * part, 16), :] = jnp.concatenate(halves, axis=1).astype(BF)

    for side in range(2):
        batch(ag, 7, r_ss.at[side, 0], r_rs.at[side, 0, 0]).wait_send()
        batch(ag.at[0], 4, r_ss.at[side, 1], r_rs.at[side, 0, 0]).wait_send()
    batch(gall, NDP - 1, d_ss.at[0], d_rs.at[0]).wait_send()

    @pl.when(own_relay)
    def _():
        batch(ks, 3, e_ss.at[0], e_rs.at[0]).wait_send()

    @pl.when(jnp.logical_not(own_relay))
    def _():
        batch(ks, 4, e_ss.at[0], e_rs.at[0]).wait_send()

    @pl.when(relay)
    def _():
        batch(ks, None, f_ss.at[0], e_rs.at[0]).wait_send()


def on_device(saved_input, grad_output, legendre, quad_weight, mixing_weight):
    hbm = pl.BlockSpec(memory_space=pltpu.HBM)
    go = grad_output[0].transpose(1, 0, 2)
    si = saved_input[0].transpose(1, 0, 2)
    vmem = pl.BlockSpec(memory_space=pltpu.VMEM)
    dma = pltpu.SemaphoreType.DMA
    gw, gi = pl.pallas_call(
        kernel,
        out_shape=(
            jax.ShapeDtypeStruct((LB, Q, Q), BF),
            jax.ShapeDtypeStruct((J, M, Q), BF),
        ),
        in_specs=[hbm, hbm, hbm, vmem, hbm],
        out_specs=(vmem, vmem),
        scratch_shapes=[
            pltpu.VMEM((J, M, Q), BF), pltpu.VMEM((J, M, Q), BF),
            pltpu.VMEM((MB, CH, 720), BF), pltpu.VMEM((LB, 512, Q), BF), dma((4,)),
            pltpu.VMEM((ROWS, ROWS), BF), pltpu.VMEM((NZ, ROWS, CH), BF),
            pltpu.VMEM((4 * CH, 16 * J), BF),
            pltpu.VMEM((ROWS, ROWS), BF), pltpu.VMEM((ROWS, ROWS), BF), pltpu.VMEM((ROWS, ROWS), BF),
            pltpu.VMEM((LB, 1024, Q), BF),
            pltpu.VMEM((NZ, CH, Q), BF), pltpu.VMEM((NZ, CH, Q), BF),
            pltpu.VMEM((ROWS, Q), F32),
            pltpu.VMEM((NZ, LB * MB, Q), BF), pltpu.VMEM((NZ, LB * MB, Q), BF),
            pltpu.VMEM((NDP, LB, M, Q), BF), pltpu.VMEM((NDP, 2, LB, M, Q), BF),
            pltpu.VMEM((NCHAN, LB, M, Q), BF), pltpu.VMEM((NCHAN, LB, M, Q), BF),
            pltpu.VMEM((2, 16, ROWS), BF), pltpu.VMEM((NZ, 16, 128), BF), pltpu.VMEM((NZ, 16, 128), BF),
            pltpu.VMEM((SHARES, NZ, 16, 128), BF), pltpu.VMEM((8, 8 * CH, 128), BF),
            pltpu.VMEM((128, 2 * CH), BF), pltpu.VMEM((8 * J, 128), BF),
            pltpu.VMEM((CH, 2 * CH), BF), pltpu.VMEM((8 * J, CH), BF),
            pltpu.VMEM((8, 2 * CH, Q), BF), pltpu.VMEM((8, CH, 2 * CH), BF), pltpu.VMEM((8, CH, Q), F32),
            pltpu.VMEM((2, NZ // 2 + 1, 8, 96, Q), BF), pltpu.VMEM((8, 8 * J, CH), BF),
            pltpu.VMEM((NZ, 8, 96, Q), BF), pltpu.VMEM((8, 8 * J, Q), F32),
            pltpu.VMEM((NDP, LB, M, Q), BF),
            dma((1,)), dma((NZ,)), dma((1,)), dma((1,)), dma((1,)), dma((1,)), dma((1,)), dma((1,)),
            dma((1,)), dma((1,)), dma((NDP,)), dma((1,)), dma((1,)), dma((1,)), dma((1,)), dma((1,)), dma((1,)), dma((1,)),
            dma((2, 2)), dma((2, NZ // 2, 4)), dma((2, 2)), dma((2, NZ // 2, 4)),
        ],
        compiler_params=pltpu.CompilerParams(
            collective_id=0, has_side_effects=True, vmem_limit_bytes=55_000_000
        ),
    )(go, si, legendre, quad_weight, mixing_weight)
    return gw, gi.transpose(1, 0, 2)[None]


def solution(mesh):
    in_specs = (
        P("dp", None, "lat", "chan"),
        P("dp", None, "lat", "chan"),
        P("lat", None, None),
        P(),
        P("lat", None, "chan"),
    )
    out_specs = (P("lat", "dp", "chan"), P("dp", None, "lat", "chan"))
    return jax.shard_map(
        on_device, mesh=mesh, in_specs=in_specs, out_specs=out_specs, check_vma=False
    )
```

```python
import jax
import jax.numpy as jnp
from jax import lax
from jax.experimental import pallas as pl
from jax.experimental.pallas import tpu as pltpu
from jax.sharding import PartitionSpec as P

MESH = pl.DeviceIdType.MESH
BF = jnp.bfloat16
F32 = jnp.float32

M, J, Q, LB, MB, CH, NZ = 64, 45, 128, 12, 4, 192, 16
ROWS = NZ * LB * MB
NCHAN, NDP = 8, 4
OROWS = 368
GROWS = 184
SHARES = 24


def iota(shape, dim):
    return lax.broadcasted_iota(jnp.int32, shape, dim)


def dot(a, b, dims=((1,), (0,))):
    return lax.dot_general(a, b, (dims, ((), ())), preferred_element_type=F32)


def static_one(hop):
    return isinstance(hop, int) and hop == 1


def one_hot(hit):
    return jnp.where(hit, 1.0, 0.0).astype(BF)


def offset_of(s):
    k = (s + 1) // 2
    far = 8 - k
    return jnp.where(s % 2 == 1, far, NZ - far)


def kernel(
    go_in, si_in, leg_in, quad, w_in, gw, gi,
    go, si, leg, w, in_sem,
    r_syn, t_syn, p_in, p_sort, p_unsort, p_merge, w2,
    g1s, g1r, acc, g2s, g2r, gall, sall, ks, kr,
    xa, tsend, trecv, tall, xr, e_col, e_row, keep_f, keep_b, x8, t_f, own, part_r, t_b, ag, oacc, gpart,
    g_ss, g_rs, g2_ss, g2_rs, k_ss, k_rs, d_ss, d_rs, e_ss, e_rs, e1_rs, f_ss,
    t_ss, t_rs, a_ss, a_rs, b_ss, b_rs, p_ss, p_rs, r_ss, r_rs,
):
    dp, z, ch = lax.axis_index("dp"), lax.axis_index("lat"), lax.axis_index("chan")
    barrier = pltpu.get_barrier_semaphore()
    loads = [
        pltpu.make_async_copy(src, dst, in_sem.at[n])
        for n, (src, dst) in enumerate(((leg_in, leg), (go_in, go), (si_in, si), (w_in, w)))
    ]
    for load in loads:
        load.start()
    g1r[:, MB * J - 4 :, :] = jnp.zeros((NZ, CH - MB * J + 4, Q), BF)

    def greet_z(s, c):
        to = (z + s + 1) % NZ
        pl.semaphore_signal(barrier, inc=1, device_id={"lat": to}, device_id_type=MESH)
        return c

    def greet_plane(s, c):
        other = (dp * NCHAN + ch + s + 1) % (NDP * NCHAN)
        pl.semaphore_signal(
            barrier, inc=1, device_id={"dp": other // NCHAN, "chan": other % NCHAN}, device_id_type=MESH
        )
        return c

    lax.fori_loop(0, NZ - 1, greet_z, 0)
    lax.fori_loop(0, NDP * NCHAN - 1, greet_plane, 0)

    def z_copy(src, dst, ss, rs, to, slot):
        return pltpu.make_async_remote_copy(
            src_ref=src.at[to], dst_ref=dst.at[slot], send_sem=ss.at[0],
            recv_sem=rs.at[slot if rs.shape[0] > 1 else 0],
            device_id={"lat": to}, device_id_type=MESH,
        )

    def z_send(src, dst, ss, rs, first, last):
        def step(s, c):
            z_copy(src, dst, ss, rs, (z + offset_of(s)) % NZ, z).start()
            return c

        lax.fori_loop(first, last, step, 0)

    def g_copy(to, slot):
        at = pl.ds(0, GROWS)
        return pltpu.make_async_remote_copy(
            src_ref=g1s.at[to, at], dst_ref=g1r.at[slot, at], send_sem=g_ss.at[0],
            recv_sem=g_rs.at[slot], device_id={"lat": to}, device_id_type=MESH,
        )

    def batch(ref, count, ss, rs):
        at = ref if count is None else ref.at[pl.ds(0, count)]
        return pltpu.make_async_remote_copy(
            src_ref=at, dst_ref=at, send_sem=ss, recv_sem=rs,
            device_id={"lat": (z + 1) % NZ}, device_id_type=MESH,
        )

    for zz in range(4):
        r, c = iota((CH, 16 * J), 0), iota((CH, 16 * J), 1)
        p_in[pl.ds(zz * CH, CH), :] = one_hot((c == (r // 4) * 16 + zz * 4 + r % 4) & (r < MB * J))

    me = dp * NCHAN + ch
    shares = me < SHARES
    group, pair = jnp.minimum(me // 2, SHARES // 2 - 1), me % 2
    loads[0].wait()
    for h in range(2):
        rows = leg[2 * pair + h, pl.ds(pl.multiple_of(16 * group, 16), 16), :].astype(F32)
        xa[h, :, 720:] = jnp.zeros((16, ROWS - 720), BF)
        xa[h, :, :720] = (rows * quad[...].reshape(1, 720)).astype(BF)

    def window(zz):
        start = jnp.minimum((zz * J) // 128, 4) * 128
        return pl.ds(pl.multiple_of(start, 128), 256), zz * J - start

    def cut(i, c):
        for u in range(4):
            zz = 4 * i + u
            at, off = window(zz)
            r, k = iota((512, 128), 0), iota((512, 128), 1)
            pick = one_hot((r % 256 == off + k % 64) & (r // 256 == k // 64) & (k % 64 < J))
            both = jnp.concatenate([xa[0, :, at], xa[1, :, at]], axis=1)
            tsend[zz] = dot(both, pick).astype(BF)
        return c

    lax.fori_loop(0, NZ // 4, cut, 0)
    loads[1].wait()
    pl.semaphore_wait(barrier, NZ - 1 + NDP * NCHAN - 1)

    def send_group(i, c):
        g = (z // 4 + 2 + i) % 4
        rows = go[:, pl.ds(pl.multiple_of(16 * g, 16), 16), :].reshape(16 * J, Q)
        g1s[pl.ds(4 * g, 4)] = dot(p_in[...], rows).astype(BF).reshape(4, CH, Q)
        for u in range(4):
            to = 4 * g + u

            @pl.when(to != z)
            def _():
                g_copy(to, z).start()

        return c

    @pl.when(shares)
    def _():
        z_send(tsend, trecv, t_ss, t_rs, 0, NZ - 1)

    lax.fori_loop(0, 4, send_group, 0)
    trecv[z] = tsend[z]
    g1r[z] = g1s[z]

    loads[2].wait()
    x8[:, 8 * J :, :] = jnp.zeros((8, CH * 2 - 8 * J, Q), BF)
    for k in range(4):
        rows = si[:, 16 * k : 16 * k + 16, :].astype(F32)
        for h in range(2):
            x8[2 * k + h, : 8 * J, :] = rows[:, 8 * h : 8 * h + 8, :].reshape(8 * J, Q).astype(BF)

    zero = jnp.zeros((ROWS, ROWS - 720), BF)
    r_syn[:, 720:] = zero

    def rows_of(ib, c):
        r = iota((128, ROWS), 0) + ib * 128
        pick = one_hot(iota((128, ROWS), 1) == (r % 4) * (NZ * LB) + r // 4)
        flat = leg[...].reshape(ROWS, 720)
        at = pl.ds(pl.multiple_of(ib * 128, 128), 128)
        r_syn[at, :720] = dot(pick, flat).astype(BF)
        return c

    lax.fori_loop(0, ROWS // 128, rows_of, 0)

    def table(src, dst):
        def step(zz, c):
            at, off = window(zz)
            r, k = iota((256, CH), 0), iota((256, CH), 1)
            pick = one_hot((r == off + k // 4) & (k < MB * J))
            full = dot(src[:, at], pick)
            keep = iota((ROWS, CH), 0) % 4 == iota((ROWS, CH), 1) % 4
            dst[zz] = jnp.where(keep, full, 0.0).astype(BF)
            return c

        lax.fori_loop(0, NZ, step, 0)

    table(r_syn, t_syn)

    def sort_block(ib, c):
        at = pl.ds(pl.multiple_of(ib * 128, 128), 128)
        r, k = iota((128, ROWS), 0) + ib * 128, iota((128, ROWS), 1)
        p_sort[at, :] = one_hot(k == ((r % M) // 4) * 48 + (r // M) * 4 + r % 4)
        p_merge[at, :] = one_hot(k == ((r % M) // 8) * 96 + (r // M) * 8 + r % 8)
        p_unsort[at, :] = one_hot(k == ((r % 96) // 8) * M + (r // 96) * 8 + r % 8)
        return c

    lax.fori_loop(0, ROWS // 128, sort_block, 0)

    r, k = iota((128, 2 * CH), 0), iota((128, 2 * CH), 1)
    e_col[...] = one_hot((r == (k % 2) * 64 + k // 8) & (k < 8 * J))
    r, k = iota((OROWS, 128), 0), iota((OROWS, 128), 1)
    e_row[...] = one_hot(k == (r % 2) * 64 + r // 8)
    keep_f[...] = one_hot(iota((CH, 2 * CH), 0) % 8 == iota((CH, 2 * CH), 1) % 8)
    keep_b[...] = one_hot(iota((OROWS, CH), 0) % 8 == iota((OROWS, CH), 1) % 8)

    ra, ca = iota((Q, Q), 0), iota((Q, Q), 1)
    swap = jnp.where(ca == ra + 1, 1.0, 0.0) * jnp.where(ra % 2 == 0, 1.0, 0.0)
    swap = (swap - jnp.where(ra == ca + 1, 1.0, 0.0) * jnp.where(ca % 2 == 0, 1.0, 0.0)).astype(BF)
    r2, c2 = iota((256, 256), 0), iota((256, 256), 1)
    weave = one_hot(c2 == (r2 % 2) * 128 + r2 // 2)

    def weave_weight(l, c):
        for k in range(4):
            block = w[l, pl.ds(128 * k, 128), :]
            both = jnp.concatenate([block, dot(block, swap).astype(BF)], axis=0)
            w2[l, pl.ds(256 * k, 256), :] = dot(weave, both).astype(BF)
        return c

    loads[3].wait()
    lax.fori_loop(0, LB // 2, weave_weight, 0)

    core = dp % 2
    sibling = dp + 1 - 2 * core

    @pl.when(shares)
    def _():
        batch(trecv, NZ - 1, t_ss.at[0], t_rs.at[0]).wait_recv()

        def a_send(s, c):
            to = ((dp // 2) * NCHAN + ch + s + 1) % (2 * NCHAN)
            pltpu.make_async_remote_copy(
                src_ref=trecv, dst_ref=tall.at[me], send_sem=a_ss.at[0], recv_sem=a_rs.at[0],
                device_id={"dp": (to // NCHAN) * 2 + core, "chan": to % NCHAN}, device_id_type=MESH,
            ).start()
            return c

        lax.fori_loop(0, 2 * NCHAN - 1, a_send, 0)
        tall[me] = trecv[...]

    lax.fori_loop(LB // 2, LB, weave_weight, 0)

    def b_copy(first):
        at = tall.at[pl.ds(first, 8)]
        return pltpu.make_async_remote_copy(
            src_ref=at, dst_ref=at, send_sem=b_ss.at[0], recv_sem=b_rs.at[0],
            device_id={"dp": sibling}, device_id_type=MESH,
        )

    def to_sibling():
        @pl.when(core == 0)
        def _():
            batch(tall, 15, a_ss.at[0], a_rs.at[0]).wait_recv()
            b_copy(0).start()
            b_copy(16).start()

        @pl.when(dp == 1)
        def _():
            batch(tall, 7, a_ss.at[0], a_rs.at[0]).wait_recv()

        @pl.when(dp == 3)
        def _():
            batch(tall, 8, a_ss.at[0], a_rs.at[0]).wait_recv()

        @pl.when(core == 1)
        def _():
            b_copy(8).start()

    acc[...] = dot(t_syn[z], g1r[z])

    def latitudes(s, c):
        frm = (z + NZ - offset_of(s)) % NZ
        g_copy(frm, frm).wait_recv()
        acc[...] += dot(t_syn[frm], g1r[frm])
        return c

    lax.fori_loop(0, 6, latitudes, 0)
    to_sibling()
    lax.fori_loop(6, NZ - 1, latitudes, 0)
    g2s[...] = acc[...].astype(BF).reshape(NZ, LB * MB, Q)
    z_send(g2s, g2r, g2_ss, g2_rs, 0, NZ - 1)
    g2r[z] = g2s[z]

    @pl.when(core == 0)
    def _():
        batch(tall, 8, b_ss.at[0], b_rs.at[0]).wait_recv()

    @pl.when(core == 1)
    def _():
        batch(tall, 16, b_ss.at[0], b_rs.at[0]).wait_recv()

    rx, cx = iota((128, 64), 0), iota((128, 64), 1)
    spread = one_hot(cx == ((rx % 8) // 2) * 16 + rx // 8)

    def by_degree(lg, c):
        at = pl.ds(pl.multiple_of(lg * 128, 128), 128)
        for g in range(8):
            tiles = [tall[2 * lg + t % 2, 2 * g + t // 2] for t in range(4)]
            xr[g, at, :] = dot(spread, jnp.concatenate(tiles, axis=0)).astype(BF)
        return c

    lax.fori_loop(0, 12, by_degree, 0)

    def both_of(g, d0, d1):
        a = xr[g, pl.ds(pl.multiple_of(d0 * 96, 32), 96), :]
        b = xr[g, pl.ds(pl.multiple_of(d1 * 96, 32), 96), :]
        return jnp.concatenate([a, b], axis=0)

    def own_terms(d0, d1):
        for g in range(8):
            t_f[g] = dot(both_of(g, d0, d1), e_col[...]).astype(BF) * keep_f[...]
        for g in range(8):
            own[g] = dot(t_f[g], x8[g])

    def p_copy(side, hop, part):
        to = (z + (1 if side == 0 else NZ - 1)) % NZ
        at = pl.ds(2 * part, 2)
        return pltpu.make_async_remote_copy(
            src_ref=part_r.at[side, hop - 1, at], dst_ref=part_r.at[side, hop, at],
            send_sem=p_ss.at[side, 0 if static_one(hop) else 1], recv_sem=p_rs.at[side, hop - 1, part],
            device_id={"lat": to}, device_id_type=MESH,
        )

    def p_send(side, hop, part, arrived):
        at = pl.ds(2 * part, 2)
        value = own[2 * part : 2 * part + 2, 96 * side : 96 * side + 96, :]
        if arrived:
            p_copy(side, hop - 1, part).wait_recv()
            value = value + part_r[side, hop - 1, at].astype(F32)
        part_r[side, hop - 1, at] = value.astype(BF)
        p_copy(side, hop, part).start()

    half_way = (z + NZ // 2) % NZ
    own_terms(half_way, half_way)
    for part in range(4):
        p_send(part // 2, 1, part, False)
    own_terms((z + 7) % NZ, (z + 9) % NZ)
    for part in range(4):
        p_send(1 - part // 2, 2, part, False)

    batch(g2r, NZ - 1, g2_ss.at[0], g2_rs.at[0]).wait_recv()
    grads = dot(p_sort[...], g2r[...].reshape(ROWS, Q)).astype(BF).reshape(LB, M, Q)
    gall[dp] = grads

    def mix(n, c):
        for l in (3 * n, 3 * n + 1, 3 * n + 2):
            full = dot(gall[dp, l], w2[l], ((1,), (1,))).astype(BF)
            for k in range(NCHAN):
                ks[k, l] = full[:, 128 * k : 128 * k + 128]
        return c

    lax.fori_loop(0, LB // 3, mix, 0)

    def k_copy(to, slot):
        return pltpu.make_async_remote_copy(
            src_ref=ks.at[to], dst_ref=kr.at[slot], send_sem=k_ss.at[0], recv_sem=k_rs.at[0],
            device_id={"chan": to}, device_id_type=MESH,
        )

    row, col = ch // 4, ch % 4
    for u in range(4):
        k_copy((1 - row) * 4 + (col + u) % 4, ch).start()
    for u in range(1, 4):
        k_copy(row * 4 + (col + u) % 4, ch).start()

    kr[ch] = ks[ch]
    for part in range(4):
        p_send(part // 2, 2, part, True)
    own_terms((z + 6) % NZ, (z + 10) % NZ)

    def ring(hop, c):
        for part in range(4):
            for side in range(2):
                p_send(side, hop, part, True)
        own_terms((z + 8 - hop) % NZ, (z + NZ - 8 + hop) % NZ)

        @pl.when(hop == 5)
        def _():
            batch(g1s.at[:, pl.ds(0, GROWS)], NZ - 1, g_ss.at[0], g_rs.at[0]).wait_send()
            batch(g2s, NZ - 1, g2_ss.at[0], g2_rs.at[0]).wait_send()

        @pl.when((hop == 6) & shares)
        def _():
            batch(tsend, NZ - 1, t_ss.at[0], t_rs.at[0]).wait_send()
            batch(tall, 15, a_ss.at[0], a_rs.at[0]).wait_send()

        @pl.when((hop == 6) & (core == 0))
        def _():
            batch(tall, 16, b_ss.at[0], b_rs.at[0]).wait_send()

        @pl.when((hop == 6) & (core == 1))
        def _():
            batch(tall, 8, b_ss.at[0], b_rs.at[0]).wait_send()

        return c

    lax.fori_loop(3, NZ // 2 + 1, ring, 0)

    batch(kr, NCHAN - 1, k_ss.at[0], k_rs.at[0]).wait_recv()

    def sum_terms(l, c):
        total = kr[0, l].astype(F32)
        for k in range(1, NCHAN):
            total = total + kr[k, l].astype(F32)
        kr[0, l] = total.astype(BF)
        return c

    lax.fori_loop(0, LB, sum_terms, 0)
    ag[z] = dot(p_unsort[...], kr[0].reshape(ROWS, Q)).astype(BF).reshape(8, 96, Q)

    def r_copy(side, hop, part, origin, last=False):
        to = (z + (1 if side == 0 else NZ - 1)) % NZ
        at = pl.ds(2 * part, 2)
        return pltpu.make_async_remote_copy(
            src_ref=ag.at[origin, at], dst_ref=ag.at[origin, at],
            send_sem=r_ss.at[side, 1 if last else 0], recv_sem=r_rs.at[side, hop, part],
            device_id={"lat": to}, device_id_type=MESH,
        )

    for part in range(4):
        for side in range(2):
            r_copy(side, 0, part, z).start()

    home, half = ch // 2, ch % 2
    relay = (col // 2) == (dp % 2)
    own_relay = home == dp
    mine = sall.at[dp, half]
    for part in range(4):
        at = pl.ds(2 * part, 2)
        value = own[2 * part : 2 * part + 2, :96, :]
        for side in range(2):
            p_copy(side, NZ // 2, part).wait_recv()
            value = value + part_r[side, NZ // 2, at].astype(F32)
        part_r[0, NZ // 2, at] = value.astype(BF)
    merged = part_r[0, NZ // 2].reshape(ROWS, Q)
    spectra = dot(p_merge[...], merged).astype(BF)
    spectra = dot(spectra, one_hot(ra == 2 * (ca % 64) + ca // 64)).astype(BF).reshape(LB, M, Q)
    s2all = ks.at[ch]
    s2all[...] = spectra

    def e_copy(src, dst, h, to, ss, rs):
        return pltpu.make_async_remote_copy(
            src_ref=src, dst_ref=dst, send_sem=ss, recv_sem=rs,
            device_id={"dp": h, "chan": to}, device_id_type=MESH,
        )

    for h in range(2):

        @pl.when(jnp.logical_not(own_relay & (row == h)))
        def _():
            e_copy(ks.at[ch], sall.at[dp, half], home, 4 * h + col, e_ss.at[0], e1_rs.at[dp]).start()

    def send_across():
        for h in range(2):
            to = 4 * h + (col + 2) % 4
            e_copy(ks.at[ch], sall.at[dp, half], home, to, e_ss.at[0], e_rs.at[0]).start()

    def d_copy(to, slot):
        return pltpu.make_async_remote_copy(
            src_ref=gall.at[dp], dst_ref=gall.at[slot], send_sem=d_ss.at[0], recv_sem=d_rs.at[0],
            device_id={"dp": to}, device_id_type=MESH,
        )

    def d_send(s, c):
        d_copy((dp + s + 1) % NDP, dp).start()
        return c

    @pl.when(own_relay)
    def _():
        mine[...] = spectra

    def pass_on():
        for b in range(NDP):
            block = sall.at[b, half]

            @pl.when(jnp.logical_not(own_relay & (dp == b)))
            def _():
                e_copy(block, block, dp, ch, f_ss.at[0], e1_rs.at[b]).wait_recv()

            for side in (1, 3):
                e_copy(block, block, dp, 4 * row + (col + side) % 4, f_ss.at[0], e_rs.at[0]).start()

    def back_terms(d0, d1):
        for g in range(8):
            t_b[g] = dot(e_row[...], both_of(g, d0, d1), ((1,), (1,))).astype(BF) * keep_b[...]

    back_terms(z, half_way)
    for g in range(8):
        oacc[g] = dot(t_b[g, :, :96], ag[z, g])
    back_terms((z + NZ - 1) % NZ, (z + 1) % NZ)

    partner_of = (-swap.astype(F32)).astype(BF)

    def hop_in(k, c):
        left, right = (z + NZ - k) % NZ, (z + k) % NZ
        for part in range(4):
            for side, origin in ((0, left), (1, right)):
                r_copy(side, k - 1, part, origin).wait_recv()
                if part // 2 == side:

                    @pl.when(k < NZ // 2 - 1)
                    def _():
                        r_copy(side, k, part, origin).start()

                    @pl.when(k == NZ // 2 - 1)
                    def _():
                        r_copy(side, k, part, origin, True).start()

                else:

                    @pl.when(k < NZ // 2 - 1)
                    def _():
                        r_copy(side, k, part, origin).start()

            for g in (2 * part, 2 * part + 1):
                oacc[g] += dot(t_b[g], jnp.concatenate([ag[left, g], ag[right, g]], axis=0))
        back_terms((z + NZ - 1 - k) % NZ, (z + 1 + k) % NZ)

        @pl.when(k == 2)
        def _():
            send_across()
            batch(kr, NCHAN - 1, k_ss.at[0], k_rs.at[0]).wait_send()
            for side in range(2):
                batch(part_r.at[side], 7, p_ss.at[side, 1], p_rs.at[side, 0, 0]).wait_send()
                batch(part_r.at[side, 0], 4, p_ss.at[side, 0], p_rs.at[side, 0, 0]).wait_send()

        @pl.when((k == 4) & relay)
        def _():
            pass_on()

        @pl.when(k == 4)
        def _():
            lax.fori_loop(0, NDP - 1, d_send, 0)

        @pl.when(k == 7)
        def _():
            batch(gall, NDP - 1, d_ss.at[0], d_rs.at[0]).wait_recv()
            for b in range(NDP):
                gpart[b] = dot(gall[b].reshape(ROWS, Q), partner_of).astype(BF).reshape(LB, M, Q)

        return c

    lax.fori_loop(1, NZ // 2, hop_in, 0)

    @pl.when(relay)
    def _():
        batch(sall, 2, e_ss.at[0], e_rs.at[0]).wait_recv()

    @pl.when(jnp.logical_not(relay))
    def _():
        batch(sall, None, e_ss.at[0], e_rs.at[0]).wait_recv()

    def weight(n, c):
        for l in (3 * n, 3 * n + 1, 3 * n + 2):
            right = jnp.concatenate(
                [jnp.concatenate([gall[b, l], gpart[b, l]], axis=1) for b in range(NDP)], axis=0
            )
            for h in range(2):
                left = jnp.concatenate([sall[b, h, l] for b in range(NDP)], axis=0)
                total = dot(left, right, ((0,), (0,)))
                gw[l, 64 * h : 64 * h + 64, :] = (
                    (total[:64, :Q] + total[64:, Q:]) * 0.25
                ).astype(BF)
        return c

    lax.fori_loop(0, LB // 3, weight, 0)

    for part in range(4):
        r_copy(part // 2, NZ // 2 - 1, part, half_way).wait_recv()
        halves = []
        for g in (2 * part, 2 * part + 1):
            full = oacc[g] + dot(t_b[g, :, :96], ag[half_way, g])
            halves.append(full[: 8 * J].reshape(J, 8, Q))
        gi[:, pl.ds(16 * part, 16), :] = jnp.concatenate(halves, axis=1).astype(BF)

    for side in range(2):
        batch(ag, 7, r_ss.at[side, 0], r_rs.at[side, 0, 0]).wait_send()
        batch(ag.at[0], 4, r_ss.at[side, 1], r_rs.at[side, 0, 0]).wait_send()
    batch(gall, NDP - 1, d_ss.at[0], d_rs.at[0]).wait_send()

    @pl.when(own_relay)
    def _():
        batch(ks, 3, e_ss.at[0], e_rs.at[0]).wait_send()

    @pl.when(jnp.logical_not(own_relay))
    def _():
        batch(ks, 4, e_ss.at[0], e_rs.at[0]).wait_send()

    @pl.when(relay)
    def _():
        batch(ks, None, f_ss.at[0], e_rs.at[0]).wait_send()


def on_device(saved_input, grad_output, legendre, quad_weight, mixing_weight):
    hbm = pl.BlockSpec(memory_space=pltpu.HBM)
    go = grad_output[0].transpose(1, 0, 2)
    si = saved_input[0].transpose(1, 0, 2)
    vmem = pl.BlockSpec(memory_space=pltpu.VMEM)
    dma = pltpu.SemaphoreType.DMA
    gw, gi = pl.pallas_call(
        kernel,
        out_shape=(
            jax.ShapeDtypeStruct((LB, Q, Q), BF),
            jax.ShapeDtypeStruct((J, M, Q), BF),
        ),
        in_specs=[hbm, hbm, hbm, vmem, hbm],
        out_specs=(vmem, vmem),
        scratch_shapes=[
            pltpu.VMEM((J, M, Q), BF), pltpu.VMEM((J, M, Q), BF),
            pltpu.VMEM((MB, CH, 720), BF), pltpu.VMEM((LB, 512, Q), BF), dma((4,)),
            pltpu.VMEM((ROWS, ROWS), BF), pltpu.VMEM((NZ, ROWS, CH), BF),
            pltpu.VMEM((4 * CH, 16 * J), BF),
            pltpu.VMEM((ROWS, ROWS), BF), pltpu.VMEM((ROWS, ROWS), BF), pltpu.VMEM((ROWS, ROWS), BF),
            pltpu.VMEM((LB, 1024, Q), BF),
            pltpu.VMEM((NZ, CH, Q), BF), pltpu.VMEM((NZ, CH, Q), BF),
            pltpu.VMEM((ROWS, Q), F32),
            pltpu.VMEM((NZ, LB * MB, Q), BF), pltpu.VMEM((NZ, LB * MB, Q), BF),
            pltpu.VMEM((NDP, LB, M, Q), BF), pltpu.VMEM((NDP, 2, LB, M, Q), BF),
            pltpu.VMEM((NCHAN, LB, M, Q), BF), pltpu.VMEM((NCHAN, LB, M, Q), BF),
            pltpu.VMEM((2, 16, ROWS), BF), pltpu.VMEM((NZ, 16, 128), BF), pltpu.VMEM((NZ, 16, 128), BF),
            pltpu.VMEM((SHARES, NZ, 16, 128), BF), pltpu.VMEM((8, 8 * CH, 128), BF),
            pltpu.VMEM((128, 2 * CH), BF), pltpu.VMEM((OROWS, 128), BF),
            pltpu.VMEM((CH, 2 * CH), BF), pltpu.VMEM((OROWS, CH), BF),
            pltpu.VMEM((8, 2 * CH, Q), BF), pltpu.VMEM((8, CH, 2 * CH), BF), pltpu.VMEM((8, CH, Q), F32),
            pltpu.VMEM((2, NZ // 2 + 1, 8, 96, Q), BF), pltpu.VMEM((8, OROWS, CH), BF),
            pltpu.VMEM((NZ, 8, 96, Q), BF), pltpu.VMEM((8, OROWS, Q), F32),
            pltpu.VMEM((NDP, LB, M, Q), BF),
            dma((1,)), dma((NZ,)), dma((1,)), dma((1,)), dma((1,)), dma((1,)), dma((1,)), dma((1,)),
            dma((1,)), dma((1,)), dma((NDP,)), dma((1,)), dma((1,)), dma((1,)), dma((1,)), dma((1,)), dma((1,)), dma((1,)),
            dma((2, 2)), dma((2, NZ // 2, 4)), dma((2, 2)), dma((2, NZ // 2, 4)),
        ],
        compiler_params=pltpu.CompilerParams(
            collective_id=0, has_side_effects=True, vmem_limit_bytes=55_000_000
        ),
    )(go, si, legendre, quad_weight, mixing_weight)
    return gw, gi.transpose(1, 0, 2)[None]


def solution(mesh):
    in_specs = (
        P("dp", None, "lat", "chan"),
        P("dp", None, "lat", "chan"),
        P("lat", None, None),
        P(),
        P("lat", None, "chan"),
    )
    out_specs = (P("lat", "dp", "chan"), P("dp", None, "lat", "chan"))
    return jax.shard_map(
        on_device, mesh=mesh, in_specs=in_specs, out_specs=out_specs, check_vma=False
    )
```
